32 devices in a mesh: rep: 2 (over x), tp: 4 (over z), sp: 4 (over y, core).
Axes of the slice: x: 2, y: 2, z: 4, core: 2. Of those that a mesh axis runs over, the one named last changes fastest.
Arguments:
- x_in: bfloat16 [8192, 5120], P(('rep', 'sp')), parts along dimension 0
- positions: int32 [8192], P(('rep', 'sp')), parts along dimension 0
- norm_gain: float32 [5120], replicated
- w_q: bfloat16 [5120, 4096], P(None, 'tp')
- w_k: bfloat16 [5120, 1024], P(None, 'tp')
- w_v: bfloat16 [5120, 1024], P(None, 'tp')
- w_o: bfloat16 [4096, 5120], P('tp')
- w_gate: bfloat16 [5120, 32768], P(None, 'tp')
- w_up: bfloat16 [5120, 32768], P(None, 'tp')
- w_down: bfloat16 [32768, 5120], P('tp')
Outputs:
- output 1: bfloat16 [8192, 5120], P(('rep', 'sp')), parts along dimension 0
- output 2: bfloat16 [8192, 16, 128], P('rep', ('tp', 'sp')), parts along dimension 0
- output 3: bfloat16 [8192, 16, 128], P('rep', ('tp', 'sp')), parts along dimension 0
There are 2 independent parts. The reference program is written for one: setup_inputs(seed, part) draws one part's arguments, and reference() takes and returns one part's arrays. A program takes and returns all parts, laid end to end along the dimension named above; an argument that names none is the same for every part.
All inputs are finite; a program needn't handle non-finite values.
Results may differ from the reference program's by a relative error of at most 0.00245318.
Values are sent between devices in bfloat16 or wider.
A program may use at most 1.25 GiB of HBM per device.

```python
import math
import jax
import jax.numpy as jnp
from jax import lax

MODEL_DIM = 5120
NUM_HEADS = 32
KV_HEADS = 8
HEAD_DIM = 128
FF_DIM = 32768
TOKENS = 4096
GROUP_DEVS = 16
DOC_COUNT = 8

KV_REPEAT = max(GROUP_DEVS // KV_HEADS, 1)
GROUP_SIZE = NUM_HEADS // KV_HEADS
ROW_BLOCK = min(TOKENS, 64)
NUM_BLOCKS = TOKENS // ROW_BLOCK
EPS = 1e-6
ROPE_BASE = 500000.0
SCORE_SCALE = 1.0 / math.sqrt(HEAD_DIM)


def setup_inputs(seed: int = 0, part: int = 0) -> dict:
    part_keys = jax.random.split(jax.random.fold_in(jax.random.key(seed), part), 3)
    shared_keys = jax.random.split(jax.random.key(seed + 1), 8)

    def weight(key_w, fan_in, fan_out):
        return (jax.random.normal(key_w, (fan_in, fan_out), jnp.float32) * fan_in ** -0.5).astype(jnp.bfloat16)

    noise_part = jax.random.normal(part_keys[0], (DOC_COUNT, TOKENS // DOC_COUNT, MODEL_DIM), jnp.float32)
    doc_means = jax.random.normal(part_keys[1], (DOC_COUNT, 1, MODEL_DIM), jnp.float32)
    x_in = (noise_part + doc_means).reshape(TOKENS, MODEL_DIM).astype(jnp.bfloat16)
    start_pos = jax.random.randint(part_keys[2], (), 0, TOKENS)
    positions = (start_pos + jnp.arange(TOKENS)).astype(jnp.int32)
    norm_gain = 1.0 + 0.3 * jax.random.normal(shared_keys[0], (MODEL_DIM,), jnp.float32)
    return {
        "x_in": x_in,
        "positions": positions,
        "norm_gain": norm_gain,
        "w_q": weight(shared_keys[1], MODEL_DIM, NUM_HEADS * HEAD_DIM),
        "w_k": weight(shared_keys[2], MODEL_DIM, KV_HEADS * HEAD_DIM),
        "w_v": weight(shared_keys[3], MODEL_DIM, KV_HEADS * HEAD_DIM),
        "w_o": weight(shared_keys[4], NUM_HEADS * HEAD_DIM, MODEL_DIM),
        "w_gate": weight(shared_keys[5], MODEL_DIM, FF_DIM),
        "w_up": weight(shared_keys[6], MODEL_DIM, FF_DIM),
        "w_down": weight(shared_keys[7], FF_DIM, MODEL_DIM),
    }


def rotate(vectors, cos_tab, sin_tab):
    half_dim = HEAD_DIM // 2
    lower_part = vectors[..., :half_dim]
    upper_part = vectors[..., half_dim:]
    return jnp.concatenate([lower_part * cos_tab - upper_part * sin_tab, upper_part * cos_tab + lower_part * sin_tab], axis=-1).astype(jnp.bfloat16)


def reference(x_in, positions, norm_gain, w_q, w_k, w_v, w_o, w_gate, w_up, w_down):
    x_f32 = x_in.astype(jnp.float32)
    inv_rms = lax.rsqrt(jnp.mean(x_f32 * x_f32, axis=-1, keepdims=True) + EPS)
    normed = (x_f32 * inv_rms * norm_gain).astype(jnp.bfloat16)
    inv_freq = ROPE_BASE ** (-(jnp.arange(HEAD_DIM // 2, dtype=jnp.float32) * (2.0 / HEAD_DIM)))
    angles = positions.astype(jnp.float32)[:, None] * inv_freq[None, :]
    cos_tab = jnp.cos(angles)[:, None, :]
    sin_tab = jnp.sin(angles)[:, None, :]
    q_rot = rotate(jnp.dot(normed, w_q, preferred_element_type=jnp.float32).reshape(TOKENS, NUM_HEADS, HEAD_DIM), cos_tab, sin_tab)
    k_rot = rotate(jnp.dot(normed, w_k, preferred_element_type=jnp.float32).reshape(TOKENS, KV_HEADS, HEAD_DIM), cos_tab, sin_tab)
    v_val = jnp.dot(normed, w_v, preferred_element_type=jnp.float32).astype(jnp.bfloat16).reshape(TOKENS, KV_HEADS, HEAD_DIM)
    q_grouped = q_rot.reshape(TOKENS, KV_HEADS, GROUP_SIZE, HEAD_DIM).astype(jnp.float32)
    k_f32 = k_rot.astype(jnp.float32)
    v_f32 = v_val.astype(jnp.float32)
    key_idx = jnp.arange(TOKENS)

    def attend_block(block_id):
        q_tile = lax.dynamic_slice_in_dim(q_grouped, block_id * ROW_BLOCK, ROW_BLOCK, axis=0)
        scores = jnp.einsum("qcgd,kcd->cgqk", q_tile, k_f32) * SCORE_SCALE
        query_idx = block_id * ROW_BLOCK + jnp.arange(ROW_BLOCK)
        scores = jnp.where(key_idx[None, :] <= query_idx[:, None], scores, -jnp.inf)
        weights = jnp.exp(scores - jnp.max(scores, axis=-1, keepdims=True))
        weight_total = jnp.sum(weights, axis=-1)
        weighted_sum = jnp.einsum("cgqk,kcd->qcgd", weights.astype(jnp.bfloat16).astype(jnp.float32), v_f32)
        return (weighted_sum / jnp.transpose(weight_total, (2, 0, 1))[..., None]).astype(jnp.bfloat16)

    attn_out = lax.map(attend_block, jnp.arange(NUM_BLOCKS)).reshape(TOKENS, NUM_HEADS * HEAD_DIM)
    attn_proj = jnp.dot(attn_out, w_o, preferred_element_type=jnp.float32)
    gate_acc = jnp.dot(normed, w_gate, preferred_element_type=jnp.float32)
    up_acc = jnp.dot(normed, w_up, preferred_element_type=jnp.float32)
    hidden = (jax.nn.silu(gate_acc) * up_acc).astype(jnp.bfloat16)
    mlp_out = jnp.dot(hidden, w_down, preferred_element_type=jnp.float32)
    y_out = (x_f32 + attn_proj + mlp_out).astype(jnp.bfloat16)
    k_cache = jnp.repeat(k_rot, KV_REPEAT, axis=1)
    v_cache = jnp.repeat(v_val, KV_REPEAT, axis=1)
    return y_out, k_cache, v_cache
```

```python
import functools

import jax
import jax.numpy as jnp
from jax import lax
from jax.experimental import pallas as pl
from jax.experimental.pallas import tpu as pltpu
from jax.sharding import PartitionSpec as P

HEAD_DIM = 128
EPS = 1e-6
ROPE_BASE = 500000.0
EXP2_SCALE = HEAD_DIM ** -0.5 * 1.4426950408889634
MESH = pl.DeviceIdType.MESH
F32 = jnp.float32
BF16 = jnp.bfloat16

SLOTS = 6
SENDS = 4
HOP = 4
BACK_HOP = 3


def block_of(size, most):
    return most if size % most == 0 else 128


def rope_tables(positions):
    inv_freq = ROPE_BASE ** (-(jnp.arange(HEAD_DIM // 2, dtype=F32) * (2.0 / HEAD_DIM)))
    angles = positions.astype(F32)[:, None] * inv_freq[None, :]
    return jnp.cos(angles)[:, None, :], jnp.sin(angles)[:, None, :]


def rotate(vectors, cos_tab, sin_tab):
    half_dim = HEAD_DIM // 2
    lower_part = vectors[..., :half_dim]
    upper_part = vectors[..., half_dim:]
    return jnp.concatenate([lower_part * cos_tab - upper_part * sin_tab, upper_part * cos_tab + lower_part * sin_tab], axis=-1).astype(BF16)


def rms_norm(x_in, gain):
    x_f32 = x_in.astype(F32)
    inv_rms = lax.rsqrt(jnp.mean(x_f32 * x_f32, axis=-1, keepdims=True) + EPS)
    return (x_f32 * inv_rms * gain).astype(BF16)


def silu_mul(gate, up):
    return (gate / (1.0 + jnp.exp(-gate)) * up).astype(BF16)


def norm_rows(src_ref, gain_ref, dst_ref, dst_row, rows):
    step = 16
    gain = gain_ref[...]

    def body(i, carry):
        base = pl.multiple_of(i * step, step)
        dst_ref[pl.ds(pl.multiple_of(dst_row + base, step), step), :] = rms_norm(src_ref[pl.ds(base, step), :], gain)
        return carry

    lax.fori_loop(0, rows // step, body, 0)


def first_hidden_kernel(core_ref, u_ref, xp_ref, gain_ref, wg_ref, wu_ref, h_ref, ubuf):
    rows = u_ref.shape[0]
    core = core_ref[0]

    @pl.when(pl.program_id(0) == 0)
    def _():
        ubuf[pl.ds(pl.multiple_of(core * rows, rows), rows), :] = u_ref[...]
        norm_rows(xp_ref, gain_ref, ubuf, (1 - core) * rows, rows)

    gate = jnp.dot(ubuf[...], wg_ref[...], preferred_element_type=F32)
    up = jnp.dot(ubuf[...], wu_ref[...], preferred_element_type=F32)
    h_ref[...] = silu_mul(gate, up)


def first_hidden(core, u_own, x_par, gain, w_gate, w_up, rows):
    model = u_own.shape[1]
    ff_half = w_gate.shape[1] // 2
    block = block_of(ff_half, 512)
    blocks = ff_half // block
    return pl.pallas_call(
        first_hidden_kernel,
        grid_spec=pltpu.PrefetchScalarGridSpec(
            num_scalar_prefetch=1,
            grid=(blocks,),
            in_specs=[
                pl.BlockSpec((rows, model), lambda i, c: (0, 0)),
                pl.BlockSpec((rows, model), lambda i, c: (0, 0)),
                pl.BlockSpec((1, model), lambda i, c: (0, 0)),
                pl.BlockSpec((model, block), lambda i, c: (0, c[0] * blocks + i)),
                pl.BlockSpec((model, block), lambda i, c: (0, c[0] * blocks + i)),
            ],
            out_specs=pl.BlockSpec((2 * rows, block), lambda i, c: (0, i)),
            scratch_shapes=[pltpu.VMEM((2 * rows, model), BF16)],
        ),
        out_shape=jax.ShapeDtypeStruct((2 * rows, ff_half), BF16),
        compiler_params=pltpu.CompilerParams(vmem_limit_bytes=56 * 2 ** 20),
        cost_estimate=pl.CostEstimate(flops=8 * rows * model * ff_half, bytes_accessed=4 * model * ff_half, transcendentals=0),
        name="first_hidden",
    )(core, u_own, x_par, gain, w_gate, w_up)


def layer_kernel(
    rows, kb_rows,
    u_own, x_own, x_par, gain_ref, q_own, q_par, kv0, kv1, kv2, kv3, h0, w_gate, w_up, w_down, w_o,
    y_out,
    wg_buf, wu_buf, wd_buf, wo_buf, ubuf, xpbuf, hbuf, abuf, qbuf, kvbuf, pbuf, rbuf, xbuf, ybuf, gbuf, m_buf, l_buf, acc_buf,
    wg_sem, wu_sem, wd_sem, wo_sem, u_sem, xp_sem, q_sem, kv_sem, h0_sem, h_send, h_recv, a_send, a_recv,
    rs_send, rs_recv, x_sem, y_near, y_far, ag_recv, ag_send, credit,
):
    tokens, model = u_own.shape
    units = tokens // rows
    ff_half = w_gate.shape[1] // 2
    cols_half = model // 2
    bg = wg_buf.shape[2]
    bw = wd_buf.shape[2]
    nbg = ff_half // bg
    nbw = cols_half // bw
    q_cols = q_own.shape[1]
    heads = q_cols // HEAD_DIM
    per_unit = 2 * nbw
    pieces = per_unit * units
    unit_ticks = 2 * nbg + 2 + 2 * nbw

    z = lax.axis_index("tp")
    nz = lax.axis_size("tp")
    sp = lax.axis_index("sp")
    core = sp % 2
    row_y = sp // 2
    partner = sp + 1 - 2 * core
    step_z = 1 - 2 * core
    hop = jnp.where(core == 0, z, nz - 1 - z)
    z_next = jnp.clip(z + step_z, 0, nz - 1)
    z_prev = jnp.clip(z - step_z, 0, nz - 1)

    barrier = pltpu.get_barrier_semaphore()
    pl.semaphore_signal(barrier, inc=1, device_id={"sp": partner}, device_id_type=MESH)

    @pl.when(z > 0)
    def _():
        pl.semaphore_signal(barrier, inc=1, device_id={"tp": z - 1}, device_id_type=MESH)
        pl.semaphore_signal(barrier, inc=1, device_id={"tp": z - 1, "sp": partner}, device_id_type=MESH)

    @pl.when(z < nz - 1)
    def _():
        pl.semaphore_signal(barrier, inc=1, device_id={"tp": z + 1}, device_id_type=MESH)
        pl.semaphore_signal(barrier, inc=1, device_id={"tp": z + 1, "sp": partner}, device_id_type=MESH)

    def mult(value, of):
        return pl.multiple_of(value, of)

    def gate_up_copies(n):
        cols = pl.ds(mult(core * ff_half + n * bg, bg), bg)
        slot = n % 2
        return (
            pltpu.make_async_copy(w_gate.at[:, cols], wg_buf.at[slot], wg_sem.at[slot]),
            pltpu.make_async_copy(w_up.at[:, cols], wu_buf.at[slot], wu_sem.at[slot]),
        )

    def start_gate_up(n):
        for copy in gate_up_copies(n):
            copy.start()

    def down_copy(n):
        b, k = n // 2, n % 2
        half = jnp.where(k == 0, core, 1 - core)
        src = w_down.at[pl.ds(mult(half * ff_half, ff_half), ff_half), pl.ds(mult(core * cols_half + b * bw, bw), bw)]
        return pltpu.make_async_copy(src, wd_buf.at[k], wd_sem.at[k])

    def out_copy(b):
        return pltpu.make_async_copy(w_o.at[:, pl.ds(mult(core * cols_half + b * bw, bw), bw)], wo_buf.at[b % 2], wo_sem.at[b % 2])

    def u_copy(u):
        return pltpu.make_async_copy(
            u_own.at[pl.ds(mult(u * rows, rows), rows), :], ubuf.at[pl.ds(mult(core * rows, rows), rows), :], u_sem)

    def xp_copy(u):
        return pltpu.make_async_copy(x_par.at[pl.ds(mult(u * rows, rows), rows), :], xpbuf, xp_sem)

    def start_q(u):
        src = pl.ds(mult(u * rows, rows), rows)
        pltpu.make_async_copy(q_own.at[src, :], qbuf.at[core], q_sem.at[0]).start()
        pltpu.make_async_copy(q_par.at[src, :], qbuf.at[1 - core], q_sem.at[1]).start()

    def wait_q():
        src = pl.ds(0, rows)
        pltpu.make_async_copy(q_own.at[src, :], qbuf.at[core], q_sem.at[0]).wait()
        pltpu.make_async_copy(q_par.at[src, :], qbuf.at[1 - core], q_sem.at[1]).wait()

    def kv_copies():
        out = []
        for d, src in enumerate((kv0, kv1, kv2, kv3)):
            source = [sp, partner, 2 * (1 - row_y) + core, 2 * (1 - row_y) + 1 - core][d]
            out.append(pltpu.make_async_copy(src, kvbuf.at[pl.ds(mult(source * tokens, tokens), tokens), :], kv_sem.at[d]))
        return out

    def h_copy(u, j):
        view = hbuf.at[u % 2, :, pl.ds(mult(core * ff_half + j * bg, bg), bg)]
        return pltpu.make_async_remote_copy(view, view, h_send.at[j], h_recv.at[u % 2, j], device_id={"sp": partner}, device_id_type=MESH)

    def h0_copy(j):
        view = hbuf.at[0, :, pl.ds(mult(core * ff_half + j * bg, bg), bg)]
        return pltpu.make_async_remote_copy(
            h0.at[:, pl.ds(mult(j * bg, bg), bg)], view, h_send.at[j], h_recv.at[0, j], device_id={"sp": partner}, device_id_type=MESH)

    def a_copy(u):
        view = abuf.at[u % 2, :, pl.ds(mult(core * q_cols, q_cols), q_cols)]
        return pltpu.make_async_remote_copy(view, view, a_send, a_recv.at[u % 2], device_id={"sp": partner}, device_id_type=MESH)

    def part(p):
        u, i = p // per_unit, p % per_unit
        return u, i // 2, i % 2

    def sum_view(p):
        u, b, r = part(p)
        return pbuf.at[u % 2, pl.ds(mult(r * rows, rows), rows), pl.ds(mult(b * bw, bw), bw)]

    def sum_copy(p):
        return pltpu.make_async_remote_copy(
            sum_view(p), rbuf.at[p % SLOTS], rs_send.at[p % SENDS], rs_recv.at[p % SLOTS], device_id={"tp": z_next}, device_id_type=MESH)

    def y_view(owner, p):
        u, b, _ = part(p)
        return y_out.at[pl.ds(mult(u * rows, rows), rows), pl.ds(mult(owner * cols_half + b * bw, bw), bw)]

    def start_x(p):
        u, b, r = part(p)
        src = (pl.ds(mult(u * rows, rows), rows), pl.ds(mult(core * cols_half + b * bw, bw), bw))

        @pl.when(r == core)
        def _():
            pltpu.make_async_copy(x_own.at[src[0], src[1]], xbuf.at[p % SENDS], x_sem.at[p % SENDS]).start()

        @pl.when(r != core)
        def _():
            pltpu.make_async_copy(x_par.at[src[0], src[1]], xbuf.at[p % SENDS], x_sem.at[p % SENDS]).start()

    def near_local(p):
        return pltpu.make_async_copy(ybuf.at[p % SENDS], y_view(core, p), y_near.at[p % SENDS])

    def near_remote(p):
        return pltpu.make_async_remote_copy(
            ybuf.at[p % SENDS], y_view(core, p), y_near.at[p % SENDS], ag_recv.at[core, p // 2], device_id={"sp": partner}, device_id_type=MESH)

    def far_remote(p):
        _, _, r = part(p)
        return pltpu.make_async_remote_copy(
            ybuf.at[p % SENDS], y_view(core, p), y_far.at[p % SENDS], ag_recv.at[core, p // 2],
            device_id={"tp": z_prev, "sp": 2 * row_y + r}, device_id_type=MESH)

    def wait_result_out(p):
        near_local(p).wait()
        far_remote(p).wait_send()

    def back_copy(owner, q):
        view = y_view(owner, 2 * q)
        z_to = jnp.clip(z - 1 + 2 * owner, 0, nz - 1)
        return pltpu.make_async_remote_copy(view, view, ag_send.at[owner, q], ag_recv.at[owner, q], device_id={"tp": z_to}, device_id_type=MESH)

    def sum_op(p):
        view = sum_view(p)

        @pl.when(hop > 0)
        def _():
            sum_copy(p).wait_recv()
            u, b, r = part(p)
            at = (u % 2, pl.ds(mult(r * rows, rows), rows), pl.ds(mult(b * bw, bw), bw))
            pbuf[at] = pbuf[at] + rbuf[p % SLOTS]

            @pl.when(p + SLOTS < pieces)
            def _():
                pl.semaphore_signal(credit, inc=1, device_id={"tp": z_prev}, device_id_type=MESH)

        @pl.when(hop < nz - 1)
        def _():
            @pl.when(p >= SENDS)
            def _():
                sum_copy(p - SENDS).wait_send()

            @pl.when(p >= SLOTS)
            def _():
                pl.semaphore_wait(credit, 1)

            sum_copy(p).start()

        @pl.when(hop == nz - 1)
        def _():
            @pl.when(p >= SENDS)
            def _():
                wait_result_out(p - SENDS)

            slot = p % SENDS
            pltpu.make_async_copy(x_own.at[pl.ds(0, rows), pl.ds(0, bw)], xbuf.at[slot], x_sem.at[slot]).wait()
            ybuf[slot] = (xbuf[slot].astype(F32) + view[...]).astype(BF16)

            @pl.when(p + 2 < pieces)
            def _():
                start_x(p + 2)

            far_remote(p).start()
            r = p % 2

            @pl.when(r == core)
            def _():
                near_local(p).start()

            @pl.when(r != core)
            def _():
                near_remote(p).start()

    def back_op(owner, q, distance):
        back_copy(owner, q).wait_recv()

        @pl.when((distance > 0) & (distance < nz - 1))
        def _():
            back_copy(owner, q).start()

    def piece_at(v):
        v_ok = jnp.maximum(v, 0)
        p = (per_unit * v_ok + unit_ticks - 1) // unit_ticks
        return p, (v >= 0) & ((unit_ticks * p) // per_unit == v_ok) & (p < pieces)

    def tick(t):
        p, here = piece_at(t - 1 - hop * HOP)

        @pl.when(here)
        def _():
            sum_op(p)

        for owner in (0, 1):
            distance = nz - 1 - z if owner == 0 else z
            pb, back = piece_at(t - 2 - (nz - 1) * HOP - distance * BACK_HOP)
            mine = (distance == 0) & (core == owner)

            @pl.when(back & (pb % 2 == core) & jnp.logical_not(mine))
            def _():
                back_op(owner, pb // 2, distance)

    last_tick = (unit_ticks * (pieces - 1)) // per_unit + 2 + (nz - 1) * (HOP + BACK_HOP)

    def attend(u, r):
        token = (2 * row_y + r) * tokens + u * rows
        q_rows = qbuf[r]
        q_stack = jnp.concatenate([q_rows[:, i * HEAD_DIM:(i + 1) * HEAD_DIM] for i in range(heads)], axis=0)
        m_buf[...] = jnp.full_like(m_buf, -jnp.inf)
        l_buf[...] = jnp.zeros_like(l_buf)
        acc_buf[...] = jnp.zeros_like(acc_buf)

        def step(kb, masked):
            base = mult(kb * kb_rows, kb_rows)
            keys = kvbuf[pl.ds(base, kb_rows), :HEAD_DIM]
            values = kvbuf[pl.ds(base, kb_rows), HEAD_DIM:]
            s = lax.dot_general(q_stack, keys, (((1,), (1,)), ((), ())), preferred_element_type=F32)
            if masked:
                row_id = token + lax.broadcasted_iota(jnp.int32, s.shape, 0) % rows
                col_id = base + lax.broadcasted_iota(jnp.int32, s.shape, 1)
                s = jnp.where(col_id <= row_id, s, -jnp.inf)
            m_old = m_buf[...]
            m_new = jnp.maximum(m_old, jnp.max(s, axis=1, keepdims=True))
            m_buf[...] = m_new
            fade = jnp.exp2((m_old - m_new) * EXP2_SCALE)
            w = jnp.exp2((s - m_new[:, :1]) * EXP2_SCALE)
            total = w[:, :128]
            for i in range(1, kb_rows // 128):
                total = total + w[:, i * 128:(i + 1) * 128]
            l_buf[...] = l_buf[...] * fade + total
            acc_buf[...] = acc_buf[...] * fade + jnp.dot(w.astype(BF16), values, preferred_element_type=F32)

        last = token // kb_rows

        def body(kb, carry):
            step(kb, False)
            return carry

        lax.fori_loop(0, last, body, 0)
        step(last, True)
        out = (acc_buf[...] / jnp.sum(l_buf[...], axis=1, keepdims=True)).astype(BF16)
        for i in range(heads):
            abuf[u % 2, pl.ds(mult(r * rows, rows), rows), pl.ds(mult(core * q_cols + i * HEAD_DIM, HEAD_DIM), HEAD_DIM)] = out[i * rows:(i + 1) * rows]

    down_copy(0).start()
    out_copy(0).start()
    down_copy(1).start()
    out_copy(1).start()
    for copy in kv_copies():
        copy.start()
    start_q(0)
    own_h0 = pltpu.make_async_copy(h0, hbuf.at[0, :, pl.ds(mult(core * ff_half, ff_half), ff_half)], h0_sem)
    own_h0.start()

    @pl.when(hop == nz - 1)
    def _():
        start_x(0)
        start_x(1)

    pl.semaphore_wait(barrier, 1 + 2 * (z > 0).astype(jnp.int32) + 2 * (z < nz - 1).astype(jnp.int32))

    def send_h0(j, carry):
        h0_copy(j).start()
        return carry

    lax.fori_loop(0, nbg, send_h0, 0)
    own_h0.wait()
    for copy in kv_copies():
        copy.wait()

    def unit(u, carry):
        t0 = u * unit_ticks

        @pl.when(u > 0)
        def _():
            down_copy(0).start()
            out_copy(0).start()
            down_copy(1).start()
            out_copy(1).start()
            xp_copy(u).wait()
            norm_rows(xpbuf, gain_ref, ubuf, (1 - core) * rows, rows)
            u_copy(u).wait()

            def gate_up(n, carry):
                slot = n % 2
                copy_g, copy_u = gate_up_copies(n)
                copy_g.wait()
                gbuf[...] = jnp.dot(ubuf[...], wg_buf[slot], preferred_element_type=F32)
                tick(t0 - 2 - 2 * nbg + 2 * n)
                copy_u.wait()
                up = jnp.dot(ubuf[...], wu_buf[slot], preferred_element_type=F32)
                hbuf[u % 2, :, pl.ds(mult(core * ff_half + n * bg, bg), bg)] = silu_mul(gbuf[...], up)

                @pl.when(n + 2 < nbg)
                def _():
                    start_gate_up(n + 2)

                tick(t0 - 2 - 2 * nbg + 2 * n + 1)
                h_copy(u, n).start()
                return carry

            lax.fori_loop(0, nbg, gate_up, 0)

        wait_q()

        def half(r, carry):
            attend(u, r)

            @pl.when(u > 0)
            def _():
                tick(t0 - 2 + r)

            return carry

        lax.fori_loop(0, 2, half, 0)
        a_copy(u).start()

        @pl.when(u + 1 < units)
        def _():
            start_q(u + 1)
            u_copy(u + 1).start()
            xp_copy(u + 1).start()
            start_gate_up(0)
            start_gate_up(1)

        def wait_h(j, carry):
            h_copy(u, j).wait()
            return carry

        def down(b, carry):
            cols = pl.ds(mult(b * bw, bw), bw)
            own_rows = pl.ds(mult(core * ff_half, ff_half), ff_half)
            par_rows = pl.ds(mult((1 - core) * ff_half, ff_half), ff_half)
            down_copy(2 * b).wait()
            pbuf[u % 2, :, cols] = jnp.dot(hbuf[u % 2, :, own_rows], wd_buf[0], preferred_element_type=F32)

            @pl.when(b + 1 < nbw)
            def _():
                down_copy(2 * b + 2).start()

            tick(t0 + 2 * b)

            @pl.when(b == 0)
            def _():
                lax.fori_loop(0, nbg, wait_h, 0)
                a_copy(u).wait()

            down_copy(2 * b + 1).wait()
            out_copy(b).wait()
            pbuf[u % 2, :, cols] = (
                pbuf[u % 2, :, cols]
                + jnp.dot(hbuf[u % 2, :, par_rows], wd_buf[1], preferred_element_type=F32)
                + jnp.dot(abuf[u % 2], wo_buf[b % 2], preferred_element_type=F32)
            )

            @pl.when(b + 1 < nbw)
            def _():
                down_copy(2 * b + 3).start()

            @pl.when(b + 2 < nbw)
            def _():
                out_copy(b + 2).start()

            tick(t0 + 2 * b + 1)
            return carry

        lax.fori_loop(0, nbw, down, 0)
        return carry

    lax.fori_loop(0, units, unit, 0)

    def drain(t, carry):
        tick(t)
        return carry

    lax.fori_loop((units - 1) * unit_ticks + 2 * nbw, last_tick + 1, drain, 0)

    def sums_out(i, carry):
        p = pieces - SENDS + i

        @pl.when(hop < nz - 1)
        def _():
            sum_copy(p).wait_send()

        @pl.when(hop == nz - 1)
        def _():
            wait_result_out(p)

        return carry

    lax.fori_loop(0, SENDS, sums_out, 0)

    for owner in (0, 1):
        distance = nz - 1 - z if owner == 0 else z

        @pl.when((distance > 0) & (distance < nz - 1))
        def _():
            def backs_out(q, carry):
                back_copy(owner, q).wait_send()
                return carry

            lax.fori_loop(0, pieces // 2, backs_out, 0)


def layer(u_own, x_own, x_par, gain, q_own, q_par, kvs, h0, w_gate, w_up, w_down, w_o, rows):
    tokens, model = u_own.shape
    ff = w_gate.shape[1]
    ff_half, cols_half = ff // 2, model // 2
    bg, bw = block_of(ff_half, 512), block_of(cols_half, 512)
    nbg, nbw = ff_half // bg, cols_half // bw
    q_cols = q_own.shape[1]
    kv_tokens = 4 * tokens
    kb_rows = min(512, kv_tokens // 2)
    pieces = 2 * nbw * (tokens // rows)
    stack = rows * (q_cols // HEAD_DIM)
    any_spec = pl.BlockSpec(memory_space=pl.ANY)
    dma = pltpu.SemaphoreType.DMA
    macs = 2 * tokens * ff_half * model * 2 + 2 * tokens * ff * cols_half + 2 * tokens * w_o.shape[0] * cols_half
    return pl.pallas_call(
        functools.partial(layer_kernel, rows, kb_rows),
        out_shape=jax.ShapeDtypeStruct((tokens, model), BF16),
        in_specs=[any_spec] * 3 + [pl.BlockSpec(memory_space=pltpu.VMEM)] + [any_spec] * 11,
        out_specs=any_spec,
        scratch_shapes=[
            pltpu.VMEM((2, model, bg), BF16),
            pltpu.VMEM((2, model, bg), BF16),
            pltpu.VMEM((2, ff_half, bw), BF16),
            pltpu.VMEM((2, w_o.shape[0], bw), BF16),
            pltpu.VMEM((2 * rows, model), BF16),
            pltpu.VMEM((rows, model), BF16),
            pltpu.VMEM((2, 2 * rows, ff), BF16),
            pltpu.VMEM((2, 2 * rows, w_o.shape[0]), BF16),
            pltpu.VMEM((2, rows, q_cols), BF16),
            pltpu.VMEM((kv_tokens, 2 * HEAD_DIM), BF16),
            pltpu.VMEM((2, 2 * rows, cols_half), F32),
            pltpu.VMEM((SLOTS, rows, bw), F32),
            pltpu.VMEM((SENDS, rows, bw), BF16),
            pltpu.VMEM((SENDS, rows, bw), BF16),
            pltpu.VMEM((2 * rows, bg), F32),
            pltpu.VMEM((stack, 128), F32),
            pltpu.VMEM((stack, 128), F32),
            pltpu.VMEM((stack, HEAD_DIM), F32),
            dma((2,)), dma((2,)), dma((2,)), dma((2,)), dma, dma, dma((2,)), dma((4,)), dma,
            dma((nbg,)), dma((2, nbg)), dma, dma((2,)),
            dma((SENDS,)), dma((SLOTS,)), dma((SENDS,)), dma((SENDS,)), dma((SENDS,)),
            dma((2, pieces // 2)), dma((2, pieces // 2)),
            pltpu.SemaphoreType.REGULAR,
        ],
        compiler_params=pltpu.CompilerParams(
            collective_id=0, has_side_effects=True, vmem_limit_bytes=67043328),
        cost_estimate=pl.CostEstimate(flops=2 * macs, bytes_accessed=6 * ff_half * model * (tokens // rows), transcendentals=0),
        name="layer",
    )(u_own, x_own, x_par, gain, q_own, q_par, *kvs, h0, w_gate, w_up, w_down, w_o)


def solution(mesh):
    row_spec = P(("rep", "sp"), None)
    cache_spec = P("rep", ("tp", "sp"), None)
    other_core = [(0, 1), (1, 0), (2, 3), (3, 2)]
    other_chip = [(0, 2), (2, 0), (1, 3), (3, 1)]
    other_both = [(0, 3), (3, 0), (1, 2), (2, 1)]

    def layer_block(x_in, positions, norm_gain, w_q, w_k, w_v, w_o, w_gate, w_up, w_down):
        tokens = x_in.shape[0]
        rows = 128 if tokens >= 1024 else tokens // 4
        heads_tp = w_q.shape[1] // HEAD_DIM
        kv_tp = w_k.shape[1] // HEAD_DIM
        core = lax.axis_index("sp") % 2
        core_arr = core.astype(jnp.int32).reshape(1)
        gain = norm_gain.reshape(1, -1)

        x_par = lax.ppermute(x_in, "sp", other_core)
        normed = rms_norm(x_in, norm_gain)
        cos_tab, sin_tab = rope_tables(positions)
        k_rot = rotate(jnp.dot(normed, w_k, preferred_element_type=F32).reshape(tokens, kv_tp, HEAD_DIM), cos_tab, sin_tab)
        v_val = jnp.dot(normed, w_v, preferred_element_type=F32).astype(BF16).reshape(tokens, kv_tp, HEAD_DIM)
        kv = jnp.concatenate([k_rot, v_val], axis=2)
        kv_mine = lax.dynamic_index_in_dim(kv, core, 1, keepdims=False)
        kv_other = lax.dynamic_index_in_dim(kv, 1 - core, 1, keepdims=False)
        kv_c = lax.ppermute(kv_mine, "sp", other_chip)
        kv_d = lax.ppermute(kv_other, "sp", other_both)
        kv_b = lax.ppermute(kv_other, "sp", other_core)
        q_rot = rotate(jnp.dot(normed, w_q, preferred_element_type=F32).reshape(tokens, heads_tp, HEAD_DIM), cos_tab, sin_tab)
        q_rot = q_rot.reshape(tokens, 2, heads_tp // 2 * HEAD_DIM)
        q_mine = lax.dynamic_index_in_dim(q_rot, core, 1, keepdims=False)
        q_other = lax.dynamic_index_in_dim(q_rot, 1 - core, 1, keepdims=False)
        q_par = lax.ppermute(q_other, "sp", other_core)

        h0 = first_hidden(core_arr, normed, x_par, gain, w_gate, w_up, rows)
        kv_late, h0 = lax.optimization_barrier((kv, h0))
        cache = lax.all_to_all(jnp.repeat(kv_late, 2, axis=1), "sp", 1, 0, tiled=True)
        y_out = layer(normed, x_in, x_par, gain, q_mine, q_par, (kv_mine, kv_b, kv_c, kv_d), h0, w_gate, w_up, w_down, w_o, rows)
        return y_out, cache[..., :HEAD_DIM], cache[..., HEAD_DIM:]

    return jax.shard_map(
        layer_block,
        mesh=mesh,
        in_specs=(row_spec, P(("rep", "sp")), P(None), P(None, "tp"), P(None, "tp"), P(None, "tp"), P("tp", None), P(None, "tp"), P(None, "tp"), P("tp", None)),
        out_specs=(row_spec, cache_spec, cache_spec),
        check_vma=False,
    )
```

```python
import functools
import math

import jax
import jax.numpy as jnp
from jax import lax
from jax.experimental import pallas as pl
from jax.experimental.pallas import tpu as pltpu
from jax.sharding import PartitionSpec as P

HEAD_DIM = 128
EPS = 1e-6
ROPE_BASE = 500000.0
EXP2_SCALE = HEAD_DIM ** -0.5 * 1.4426950408889634
MESH = pl.DeviceIdType.MESH
F32 = jnp.float32
BF16 = jnp.bfloat16

SLOTS = 8
SENDS = 4
HOP = 4
BACK_HOP = 3
DOWN_SLOTS = 2


def block_of(size, most):
    return most if size % most == 0 else most // 2


def over(x, d):
    if d & (d - 1) == 0:
        return lax.shift_right_logical(x, d.bit_length() - 1)
    return lax.shift_right_logical(x * (65536 // d + 1), 16)


def rope_tables(positions):
    inv_freq = ROPE_BASE ** (-(jnp.arange(HEAD_DIM // 2, dtype=F32) * (2.0 / HEAD_DIM)))
    angles = positions.astype(F32)[:, None] * jnp.concatenate([inv_freq, inv_freq])[None, :]
    sign = jnp.where(jnp.arange(HEAD_DIM) < HEAD_DIM // 2, -1.0, 1.0)
    return jnp.cos(angles), jnp.sin(angles) * sign[None, :]


def rotate(vectors, cos_tab, sin_tab):
    return (vectors * cos_tab + pltpu.roll(vectors, HEAD_DIM // 2, 1) * sin_tab).astype(BF16)


def rms_norm(x_in, gain):
    x_f32 = x_in.astype(F32)
    inv_rms = lax.rsqrt(jnp.mean(x_f32 * x_f32, axis=-1, keepdims=True) + EPS)
    return (x_f32 * inv_rms * gain).astype(BF16)


def silu_mul(gate, up):
    return (gate / (1.0 + jnp.exp(-gate)) * up).astype(BF16)


def qkv_kernel(core_ref, x_ref, gain_ref, cos_ref, sin_ref, wk_ref, wv_ref, wq_ref, u_ref, kv_ref, vt_ref, q_other_ref, q_mine_ref, u_buf):
    phase, block = pl.program_id(0), pl.program_id(1)
    rows = x_ref.shape[0]
    at = pl.ds(pl.multiple_of(block * rows, rows), rows)

    @pl.when(phase == 0)
    def _():
        step = 16

        def norm(i, carry):
            part = pl.ds(pl.multiple_of(i * step, step), step)
            u_ref[part, :] = rms_norm(x_ref[part, :], gain_ref[...])
            return carry

        lax.fori_loop(0, rows // step, norm, 0)
        u_buf[at, :] = u_ref[...]
        k = jnp.dot(u_ref[...], wk_ref[...], preferred_element_type=F32)
        v = jnp.dot(u_ref[...], wv_ref[...], preferred_element_type=F32)
        for head in range(2):
            cols = slice(head * HEAD_DIM, (head + 1) * HEAD_DIM)
            kv_ref[head, :, :HEAD_DIM] = rotate(k[:, cols], cos_ref[at, :], sin_ref[at, :])
            kv_ref[head, :, HEAD_DIM:] = v[:, cols].astype(BF16)
            vt_ref[head] = v[:, cols].T.astype(BF16)

    def queries(q_ref):
        q = jnp.dot(u_buf[at, :], wq_ref[...], preferred_element_type=F32)
        for head in range(q.shape[1] // HEAD_DIM):
            cols = slice(head * HEAD_DIM, (head + 1) * HEAD_DIM)
            q_ref[:, cols] = rotate(q[:, cols], cos_ref[at, :], sin_ref[at, :])

    pl.when(phase == 1)(lambda: queries(q_other_ref))
    pl.when(phase == 2)(lambda: queries(q_mine_ref))


def project(core, x_in, gain, cos_tab, sin_tab, w_k, w_v, w_q):
    tokens, model = x_in.shape
    rows = min(256, tokens // 2)
    blocks = tokens // rows
    q_cols = w_q.shape[1] // 2
    last = blocks - 1

    def first(p, i):
        return jnp.where(p == 0, i, last)

    return pl.pallas_call(
        qkv_kernel,
        grid_spec=pltpu.PrefetchScalarGridSpec(
            num_scalar_prefetch=1,
            grid=(3, blocks),
            in_specs=[
                pl.BlockSpec((rows, model), lambda p, i, c: (first(p, i), 0)),
                pl.BlockSpec((1, model), lambda p, i, c: (0, 0)),
                pl.BlockSpec((tokens, HEAD_DIM), lambda p, i, c: (0, 0)),
                pl.BlockSpec((tokens, HEAD_DIM), lambda p, i, c: (0, 0)),
                pl.BlockSpec((model, 2 * HEAD_DIM), lambda p, i, c: (0, 0)),
                pl.BlockSpec((model, 2 * HEAD_DIM), lambda p, i, c: (0, 0)),
                pl.BlockSpec((model, q_cols), lambda p, i, c: (0, jnp.where(p == 2, c[0], 1 - c[0]))),
            ],
            out_specs=[
                pl.BlockSpec((rows, model), lambda p, i, c: (first(p, i), 0)),
                pl.BlockSpec((2, rows, 2 * HEAD_DIM), lambda p, i, c: (0, first(p, i), 0)),
                pl.BlockSpec((2, HEAD_DIM, rows), lambda p, i, c: (0, 0, first(p, i))),
                pl.BlockSpec((rows, q_cols), lambda p, i, c: (jnp.where(p == 0, 0, jnp.where(p == 1, i, last)), 0)),
                pl.BlockSpec((rows, q_cols), lambda p, i, c: (jnp.where(p == 2, i, 0), 0)),
            ],
            scratch_shapes=[pltpu.VMEM((tokens, model), BF16)],
        ),
        out_shape=[
            jax.ShapeDtypeStruct((tokens, model), BF16),
            jax.ShapeDtypeStruct((2, tokens, 2 * HEAD_DIM), BF16),
            jax.ShapeDtypeStruct((2, HEAD_DIM, tokens), BF16),
            jax.ShapeDtypeStruct((tokens, q_cols), BF16),
            jax.ShapeDtypeStruct((tokens, q_cols), BF16),
        ],
        compiler_params=pltpu.CompilerParams(vmem_limit_bytes=60 * 2 ** 20),
        cost_estimate=pl.CostEstimate(flops=2 * tokens * model * (2 * q_cols + 4 * HEAD_DIM), bytes_accessed=6 * tokens * model, transcendentals=0),
        name="project",
    )(core, x_in, gain, cos_tab, sin_tab, w_k, w_v, w_q)


def layer_kernel(
    rows, att, keys_step,
    u_own, x_own, x_par, q_mine, q_other, kv, vt, w_gate, w_up, w_down, w_o,
    y_out, cache, u_par,
    wgu_buf, wd_buf, wo_buf, ubuf, hbuf, abuf, qbuf, kbuf, vtbuf, pbuf, rbuf, xbuf, ybuf, m_buf, l_buf, acc_buf,
    wgu_sem, wd_sem, wo_sem, u_sem, near_sem, u_send, u_recv, q_send, q_recv, kv_send, kv_recv,
    h_send, h_recv, a_send, a_recv, rs_send, rs_recv, x_sem, y_near, y_far, ag_recv, ag_send, credit,
):
    tokens, model = u_own.shape
    units = tokens // rows
    ff_half = w_gate.shape[1] // 2
    cols_half = model // 2
    bg = wgu_buf.shape[2] // 2
    wb = wd_buf.shape[2]
    bw = wb // 2
    nbg = ff_half // bg
    nbw = cols_half // bw
    q_cols = q_mine.shape[1]
    heads = q_cols // HEAD_DIM
    subs = rows // att
    per_unit = 2 * nbw
    pieces = per_unit * units
    unit_ticks = 2 * nbg + 2 * subs + 2 * nbw

    z = lax.axis_index("tp")
    nz = lax.axis_size("tp")
    sp = lax.axis_index("sp")
    core = sp % 2
    row_y = sp // 2
    partner = sp + 1 - 2 * core
    across = 2 * (1 - row_y) + core
    across_partner = 2 * (1 - row_y) + 1 - core
    step_z = 1 - 2 * core
    hop = jnp.where(core == 0, z, nz - 1 - z)
    z_next = jnp.clip(z + step_z, 0, nz - 1)
    z_prev = jnp.clip(z - step_z, 0, nz - 1)

    def mult(value, of):
        return pl.multiple_of(value, of)

    def gate_up_copies(n):
        cols = pl.ds(mult(core * ff_half + n * bg, bg), bg)
        slot = n & 1
        return (
            pltpu.make_async_copy(w_gate.at[:, cols], wgu_buf.at[slot, :, pl.ds(0, bg)], wgu_sem.at[slot, 0]),
            pltpu.make_async_copy(w_up.at[:, cols], wgu_buf.at[slot, :, pl.ds(bg, bg)], wgu_sem.at[slot, 1]),
        )

    def start_gate_up(n):
        for copy in gate_up_copies(n):
            copy.start()

    def down_copy(n):
        b, k = n // 2, n % 2
        half = jnp.where(k == 0, core, 1 - core)
        src = w_down.at[pl.ds(mult(half * ff_half, ff_half), ff_half), pl.ds(mult(core * cols_half + b * wb, wb), wb)]
        slot = n % DOWN_SLOTS
        return pltpu.make_async_copy(src, wd_buf.at[slot], wd_sem.at[slot])

    def out_copy(b):
        return pltpu.make_async_copy(w_o.at[:, pl.ds(mult(core * cols_half + b * wb, wb), wb)], wo_buf.at[b & 1], wo_sem.at[b & 1])

    def u_rows(u):
        return pl.ds(mult(u * rows, rows), rows)

    def own_u_copy(u):
        return pltpu.make_async_copy(u_own.at[u_rows(u), :], ubuf.at[u_rows(core), :], u_sem.at[0])

    def par_u_copy(u):
        return pltpu.make_async_copy(u_par.at[u_rows(u), :], ubuf.at[u_rows(1 - core), :], u_sem.at[1])

    own_tokens = pl.ds(mult(sp * tokens, tokens), tokens)

    def own_copies():
        return (
            pltpu.make_async_copy(q_mine, qbuf.at[core], near_sem.at[0]),
            pltpu.make_async_copy(kv.at[core, :, pl.ds(0, HEAD_DIM)], kbuf.at[own_tokens, :], near_sem.at[1]),
            pltpu.make_async_copy(vt.at[core], vtbuf.at[:, own_tokens], near_sem.at[2]),
        )

    def own_cache():
        return pltpu.make_async_copy(kv.at[row_y], cache.at[own_tokens, :], near_sem.at[3])

    def h_copy(u, j):
        view = hbuf.at[u & 1, :, pl.ds(mult(core * ff_half + j * bg, bg), bg)]
        return pltpu.make_async_remote_copy(view, view, h_send.at[j], h_recv.at[u & 1, j], device_id={"sp": partner}, device_id_type=MESH)

    def first_u_copy():
        return pltpu.make_async_remote_copy(
            u_own.at[u_rows(0), :], ubuf.at[u_rows(core), :], u_send.at[0], u_recv.at[0], device_id={"sp": partner}, device_id_type=MESH)

    def far_u_copy(u):
        return pltpu.make_async_remote_copy(
            u_own.at[u_rows(u), :], u_par.at[u_rows(u), :], u_send.at[u], u_recv.at[u], device_id={"sp": partner}, device_id_type=MESH)

    def q_copy():
        return pltpu.make_async_remote_copy(q_other, qbuf.at[core], q_send, q_recv, device_id={"sp": partner}, device_id_type=MESH)

    peers = ((partner, 1 - core, row_y), (across, core, 1 - row_y), (across_partner, 1 - core, 1 - row_y))

    def key_copies(d):
        to, head, _ = peers[d]
        return (
            pltpu.make_async_remote_copy(
                kv.at[head, :, pl.ds(0, HEAD_DIM)], kbuf.at[own_tokens, :], kv_send.at[0, d], kv_recv.at[0, d], device_id={"sp": to}, device_id_type=MESH),
            pltpu.make_async_remote_copy(
                vt.at[head], vtbuf.at[:, own_tokens], kv_send.at[1, d], kv_recv.at[1, d], device_id={"sp": to}, device_id_type=MESH),
        )

    def cache_copy(d):
        to, _, head = peers[d]
        return pltpu.make_async_remote_copy(
            kv.at[head], cache.at[own_tokens, :], kv_send.at[2, d], kv_recv.at[2, d], device_id={"sp": to}, device_id_type=MESH)

    def a_copy(u):
        view = abuf.at[u & 1, :, pl.ds(mult(core * q_cols, q_cols), q_cols)]
        return pltpu.make_async_remote_copy(view, view, a_send, a_recv.at[u & 1], device_id={"sp": partner}, device_id_type=MESH)

    def part(p):
        u = over(p, per_unit)
        i = p - u * per_unit
        return u, lax.shift_right_logical(i, 1), i & 1

    def sum_view(p):
        u, b, r = part(p)
        return pbuf.at[u & 1, pl.ds(mult(r * rows, rows), rows), pl.ds(mult(b * bw, bw), bw)]

    def sum_copy(p):
        return pltpu.make_async_remote_copy(
            sum_view(p), rbuf.at[p & (SLOTS - 1)], rs_send.at[p & (SENDS - 1)], rs_recv.at[p & (SLOTS - 1)], device_id={"tp": z_next}, device_id_type=MESH)

    def y_view(owner, p):
        u, b, _ = part(p)
        return y_out.at[pl.ds(mult(u * rows, rows), rows), pl.ds(mult(owner * cols_half + b * bw, bw), bw)]

    def start_x(p):
        u, b, r = part(p)
        src = (pl.ds(mult(u * rows, rows), rows), pl.ds(mult(core * cols_half + b * bw, bw), bw))

        @pl.when(r == core)
        def _():
            pltpu.make_async_copy(x_own.at[src[0], src[1]], xbuf.at[p & (SENDS - 1)], x_sem.at[p & (SENDS - 1)]).start()

        @pl.when(r != core)
        def _():
            pltpu.make_async_copy(x_par.at[src[0], src[1]], xbuf.at[p & (SENDS - 1)], x_sem.at[p & (SENDS - 1)]).start()

    def near_local(p):
        return pltpu.make_async_copy(ybuf.at[p & (SENDS - 1)], y_view(core, p), y_near.at[p & (SENDS - 1)])

    def near_remote(p):
        return pltpu.make_async_remote_copy(
            ybuf.at[p & (SENDS - 1)], y_view(core, p), y_near.at[p & (SENDS - 1)], ag_recv.at[core, lax.shift_right_logical(p, 1)], device_id={"sp": partner}, device_id_type=MESH)

    def far_remote(p):
        _, _, r = part(p)
        return pltpu.make_async_remote_copy(
            ybuf.at[p & (SENDS - 1)], y_view(core, p), y_far.at[p & (SENDS - 1)], ag_recv.at[core, lax.shift_right_logical(p, 1)],
            device_id={"tp": z_prev, "sp": 2 * row_y + r}, device_id_type=MESH)

    def wait_result_out(p):
        near_local(p).wait()
        far_remote(p).wait_send()

    def back_copy(owner, q):
        view = y_view(owner, 2 * q)
        z_to = jnp.clip(z - 1 + 2 * owner, 0, nz - 1)
        return pltpu.make_async_remote_copy(view, view, ag_send.at[owner, q], ag_recv.at[owner, q], device_id={"tp": z_to}, device_id_type=MESH)

    def sum_op(p):
        view = sum_view(p)

        @pl.when(hop > 0)
        def _():
            sum_copy(p).wait_recv()
            u, b, r = part(p)
            at = (u & 1, pl.ds(mult(r * rows, rows), rows), pl.ds(mult(b * bw, bw), bw))
            pbuf[at] = pbuf[at] + rbuf[p & (SLOTS - 1)]

            @pl.when(p + SLOTS < pieces)
            def _():
                pl.semaphore_signal(credit, inc=1, device_id={"tp": z_prev}, device_id_type=MESH)

        @pl.when(hop < nz - 1)
        def _():
            @pl.when(p >= SENDS)
            def _():
                sum_copy(p - SENDS).wait_send()

            @pl.when(p >= SLOTS)
            def _():
                pl.semaphore_wait(credit, 1)

            sum_copy(p).start()

        @pl.when(hop == nz - 1)
        def _():
            @pl.when(p >= SENDS)
            def _():
                wait_result_out(p - SENDS)

            slot = p & (SENDS - 1)
            pltpu.make_async_copy(x_own.at[pl.ds(0, rows), pl.ds(0, bw)], xbuf.at[slot], x_sem.at[slot]).wait()
            ybuf[slot] = (xbuf[slot].astype(F32) + view[...]).astype(BF16)

            @pl.when(p + 2 < pieces)
            def _():
                start_x(p + 2)

            far_remote(p).start()
            r = p & 1

            @pl.when(r == core)
            def _():
                near_local(p).start()

            @pl.when(r != core)
            def _():
                near_remote(p).start()

    def back_op(owner, q, distance):
        back_copy(owner, q).wait_recv()

        @pl.when((distance > 0) & (distance < nz - 1))
        def _():
            back_copy(owner, q).start()

    def ticks(t, count):
        def body(i, carry):
            tick(t + i)
            return carry

        lax.fori_loop(0, count, body, 0)

    shrink = math.gcd(per_unit, unit_ticks)
    rate = per_unit // shrink, unit_ticks // shrink

    def piece_at(v):
        v_ok = jnp.maximum(v, 0)
        p = over(rate[0] * v_ok + rate[1] - 1, rate[1])
        return p, (v >= 0) & (over(rate[1] * p, rate[0]) == v_ok) & (p < pieces)

    def tick(t):
        p, here = piece_at(t - 2 - hop * HOP)

        @pl.when(here)
        def _():
            sum_op(p)

        for owner in (0, 1):
            distance = nz - 1 - z if owner == 0 else z
            pb, back = piece_at(t - 3 - (nz - 1) * HOP - distance * BACK_HOP)
            mine = (distance == 0) & (core == owner)

            @pl.when(back & ((pb & 1) == core) & jnp.logical_not(mine))
            def _():
                back_op(owner, lax.shift_right_logical(pb, 1), distance)

    last_tick = (rate[1] * (pieces - 1)) // rate[0] + 3 + (nz - 1) * (HOP + BACK_HOP)

    def attend(u, r, s):
        first = u * rows + s * att
        token = (2 * row_y + r) * tokens + first
        q_rows = qbuf[r, pl.ds(mult(first, att), att), :]
        q_stack = jnp.concatenate([q_rows[:, i * HEAD_DIM:(i + 1) * HEAD_DIM] for i in range(heads)], axis=0)
        m_buf[...] = jnp.full_like(m_buf, -jnp.inf)
        l_buf[...] = jnp.zeros_like(l_buf)
        acc_buf[...] = jnp.zeros_like(acc_buf)

        def step(base, count, masked):
            starts = [mult(base + j * keys_step, keys_step) for j in range(count)]
            scores = []
            for start in starts:
                part = lax.dot_general(kbuf[pl.ds(start, keys_step), :], q_stack, (((1,), (1,)), ((), ())), preferred_element_type=F32)
                if masked:
                    key_id = start + lax.broadcasted_iota(jnp.int32, part.shape, 0)
                    token_id = token + (lax.broadcasted_iota(jnp.int32, part.shape, 1) & (att - 1))
                    part = jnp.where(key_id <= token_id, part, -jnp.inf)
                scores.append(part)
            m_old = m_buf[...]
            m_new = m_old
            for part in scores:
                m_new = jnp.maximum(m_new, jnp.max(part, axis=0, keepdims=True))
            m_buf[...] = m_new
            fade = jnp.exp2((m_old - m_new) * EXP2_SCALE)
            total, mixed = None, None
            for start, part in zip(starts, scores):
                w = jnp.exp2((part - m_new[0:1]) * EXP2_SCALE)
                w_sum = jnp.sum(w.reshape(keys_step // 8, 8, w.shape[1]), axis=0)
                w_v = jnp.dot(vtbuf[:, pl.ds(start, keys_step)], w.astype(BF16), preferred_element_type=F32)
                total = w_sum if total is None else total + w_sum
                mixed = w_v if mixed is None else mixed + w_v
            l_buf[...] = l_buf[...] * fade + total
            acc_buf[...] = acc_buf[...] * fade[0:1] + mixed

        span = 2 * keys_step
        spans = token // span

        def clear(i, carry):
            step(i * span, 2, False)
            return carry

        def edge(i, carry):
            step(spans * span + i * keys_step, 1, True)
            return carry

        lax.fori_loop(0, spans, clear, 0)
        lax.fori_loop(0, (token - spans * span) // keys_step + 1, edge, 0)
        out = (acc_buf[...] / jnp.sum(l_buf[...], axis=0, keepdims=True)).astype(BF16)
        for i in range(heads):
            abuf[u & 1, pl.ds(mult(r * rows + s * att, att), att), pl.ds(mult(core * q_cols + i * HEAD_DIM, HEAD_DIM), HEAD_DIM)] = out[:, i * att:(i + 1) * att].T

    start_gate_up(0)
    own_u_copy(0).start()
    start_gate_up(1)
    for copy in own_copies():
        copy.start()
    own_cache().start()

    @pl.when(hop == nz - 1)
    def _():
        start_x(0)
        start_x(1)

    barrier = pltpu.get_barrier_semaphore()
    for other in (partner, across, across_partner):
        pl.semaphore_signal(barrier, inc=1, device_id={"sp": other}, device_id_type=MESH)

    @pl.when(z > 0)
    def _():
        pl.semaphore_signal(barrier, inc=1, device_id={"tp": z - 1}, device_id_type=MESH)
        pl.semaphore_signal(barrier, inc=1, device_id={"tp": z - 1, "sp": partner}, device_id_type=MESH)

    @pl.when(z < nz - 1)
    def _():
        pl.semaphore_signal(barrier, inc=1, device_id={"tp": z + 1}, device_id_type=MESH)
        pl.semaphore_signal(barrier, inc=1, device_id={"tp": z + 1, "sp": partner}, device_id_type=MESH)

    pl.semaphore_wait(barrier, 3 + 2 * (z > 0).astype(jnp.int32) + 2 * (z < nz - 1).astype(jnp.int32))

    first_u_copy().start()
    for d in (1, 2, 0):
        for copy in key_copies(d):
            copy.start()
    q_copy().start()

    def send_u(u, carry):
        far_u_copy(u).start()
        return carry

    lax.fori_loop(1, units, send_u, 0)

    def unit(u, carry):
        t0 = u * unit_ticks
        gate_up_tick = t0 - 2 * nbg - 2 * subs
        own_u_copy(u).wait()

        @pl.when(u == 0)
        def _():
            first_u_copy().wait()

        @pl.when(u > 0)
        def _():
            par_u_copy(u).wait()

        for n in range(DOWN_SLOTS):
            down_copy(n).start()
        out_copy(0).start()
        out_copy(1).start()

        def gate_up(n, carry):
            slot = n & 1
            copy_g, copy_u = gate_up_copies(n)
            copy_g.wait()
            copy_u.wait()
            both = jnp.dot(ubuf[...], wgu_buf[slot], preferred_element_type=F32)
            hbuf[u & 1, :, pl.ds(mult(core * ff_half + n * bg, bg), bg)] = silu_mul(both[:, :bg], both[:, bg:])

            @pl.when(n + 2 < nbg)
            def _():
                start_gate_up(n + 2)

            ticks(gate_up_tick + 2 * n, 2)
            h_copy(u, n).start()
            return carry

        lax.fori_loop(0, nbg, gate_up, 0)

        @pl.when(u == 0)
        def _():
            for copy in own_copies():
                copy.wait()
            for d in range(3):
                for copy in key_copies(d):
                    copy.wait()
            q_copy().wait()
            for d in range(3):
                cache_copy(d).start()

        def sub(i, carry):
            r = over(i, subs)
            attend(u, r, i - r * subs)
            tick(t0 - 2 * subs + i)
            return carry

        lax.fori_loop(0, 2 * subs, sub, 0)
        a_copy(u).start()

        @pl.when(u + 1 < units)
        def _():
            own_u_copy(u + 1).start()
            far_u_copy(u + 1).wait()
            par_u_copy(u + 1).start()
            start_gate_up(0)
            start_gate_up(1)

        def wait_h(j, carry):
            h_copy(u, j).wait()
            return carry

        def down(b, carry):
            cols = pl.ds(mult(b * wb, wb), wb)
            own_rows = pl.ds(mult(core * ff_half, ff_half), ff_half)
            par_rows = pl.ds(mult((1 - core) * ff_half, ff_half), ff_half)
            down_copy(2 * b).wait()
            pbuf[u & 1, :, cols] = jnp.dot(hbuf[u & 1, :, own_rows], wd_buf[0], preferred_element_type=F32)

            @pl.when(b + 1 < nbw // 2)
            def _():
                down_copy(2 * b + 2).start()

            ticks(t0 + 4 * b, 2)

            @pl.when(b == 0)
            def _():
                lax.fori_loop(0, nbg, wait_h, 0)
                a_copy(u).wait()

            down_copy(2 * b + 1).wait()
            out_copy(b).wait()
            pbuf[u & 1, :, cols] = (
                pbuf[u & 1, :, cols]
                + jnp.dot(hbuf[u & 1, :, par_rows], wd_buf[1], preferred_element_type=F32)
                + jnp.dot(abuf[u & 1], wo_buf[b & 1], preferred_element_type=F32)
            )

            @pl.when(b + 1 < nbw // 2)
            def _():
                down_copy(2 * b + 3).start()

            @pl.when(b + 2 < nbw // 2)
            def _():
                out_copy(b + 2).start()

            ticks(t0 + 4 * b + 2, 2)
            return carry

        lax.fori_loop(0, nbw // 2, down, 0)
        return carry

    lax.fori_loop(0, units, unit, 0)

    def drain(t, carry):
        tick(t)
        return carry

    lax.fori_loop((units - 1) * unit_ticks + 2 * nbw, last_tick + 1, drain, 0)

    def sums_out(i, carry):
        p = pieces - SENDS + i

        @pl.when(hop < nz - 1)
        def _():
            sum_copy(p).wait_send()

        @pl.when(hop == nz - 1)
        def _():
            wait_result_out(p)

        return carry

    lax.fori_loop(0, SENDS, sums_out, 0)

    for owner in (0, 1):
        distance = nz - 1 - z if owner == 0 else z

        @pl.when((distance > 0) & (distance < nz - 1))
        def _():
            def backs_out(q, carry):
                back_copy(owner, q).wait_send()
                return carry

            lax.fori_loop(0, pieces // 2, backs_out, 0)

    own_cache().wait()
    for d in range(3):
        cache_copy(d).wait()


def layer(u_own, x_own, x_par, q_mine, q_other, kv, vt, w_gate, w_up, w_down, w_o):
    tokens, model = u_own.shape
    ff = w_gate.shape[1]
    ff_half, cols_half = ff // 2, model // 2
    rows = tokens // 4
    att = min(128, rows)
    bg, bw = block_of(ff_half, 256), block_of(cols_half, 512) // 2
    wb = 2 * bw
    nbg, nbw = ff_half // bg, cols_half // bw
    q_cols = q_mine.shape[1]
    kv_tokens = 4 * tokens
    keys_step = min(512, kv_tokens // 4)
    units = tokens // rows
    pieces = 2 * nbw * units
    stack = att * (q_cols // HEAD_DIM)
    any_spec = pl.BlockSpec(memory_space=pl.ANY)
    dma = pltpu.SemaphoreType.DMA
    macs = 2 * tokens * ff_half * model * 2 + 2 * tokens * ff * cols_half + 2 * tokens * w_o.shape[0] * cols_half
    y_out, cache, _ = pl.pallas_call(
        functools.partial(layer_kernel, rows, att, keys_step),
        out_shape=[
            jax.ShapeDtypeStruct((tokens, model), BF16),
            jax.ShapeDtypeStruct((kv_tokens, 2 * HEAD_DIM), BF16),
            jax.ShapeDtypeStruct((tokens, model), BF16),
        ],
        in_specs=[any_spec] * 11,
        out_specs=[any_spec] * 3,
        scratch_shapes=[
            pltpu.VMEM((2, model, 2 * bg), BF16),
            pltpu.VMEM((DOWN_SLOTS, ff_half, wb), BF16),
            pltpu.VMEM((2, w_o.shape[0], wb), BF16),
            pltpu.VMEM((2 * rows, model), BF16),
            pltpu.VMEM((2, 2 * rows, ff), BF16),
            pltpu.VMEM((2, 2 * rows, w_o.shape[0]), BF16),
            pltpu.VMEM((2, tokens, q_cols), BF16),
            pltpu.VMEM((kv_tokens, HEAD_DIM), BF16),
            pltpu.VMEM((HEAD_DIM, kv_tokens), BF16),
            pltpu.VMEM((2, 2 * rows, cols_half), F32),
            pltpu.VMEM((SLOTS, rows, bw), F32),
            pltpu.VMEM((SENDS, rows, bw), BF16),
            pltpu.VMEM((SENDS, rows, bw), BF16),
            pltpu.VMEM((8, stack), F32),
            pltpu.VMEM((8, stack), F32),
            pltpu.VMEM((HEAD_DIM, stack), F32),
            dma((2, 2)), dma((DOWN_SLOTS,)), dma((2,)), dma((2,)), dma((4,)), dma((units,)), dma((units,)), dma, dma, dma((3, 3)), dma((3, 3)),
            dma((nbg,)), dma((2, nbg)), dma, dma((2,)),
            dma((SENDS,)), dma((SLOTS,)), dma((SENDS,)), dma((SENDS,)), dma((SENDS,)),
            dma((2, pieces // 2)), dma((2, pieces // 2)),
            pltpu.SemaphoreType.REGULAR,
        ],
        compiler_params=pltpu.CompilerParams(
            collective_id=0, has_side_effects=True, vmem_limit_bytes=67043328),
        cost_estimate=pl.CostEstimate(flops=2 * macs, bytes_accessed=6 * ff_half * model * units, transcendentals=0),
        name="layer",
    )(u_own, x_own, x_par, q_mine, q_other, kv, vt, w_gate, w_up, w_down, w_o)
    return y_out, cache


def solution(mesh):
    row_spec = P(("rep", "sp"), None)
    cache_spec = P("rep", ("tp", "sp"), None)
    other_core = [(0, 1), (1, 0), (2, 3), (3, 2)]

    def layer_block(x_in, positions, norm_gain, w_q, w_k, w_v, w_o, w_gate, w_up, w_down):
        core = (lax.axis_index("sp") % 2).astype(jnp.int32).reshape(1)
        x_par = lax.ppermute(x_in, "sp", other_core)
        cos_tab, sin_tab = rope_tables(positions)
        normed, kv, vt, q_other, q_mine = project(core, x_in, norm_gain.reshape(1, -1), cos_tab, sin_tab, w_k, w_v, w_q)
        y_out, cache = layer(normed, x_in, x_par, q_mine, q_other, kv, vt, w_gate, w_up, w_down, w_o)
        return y_out, cache[:, None, :HEAD_DIM], cache[:, None, HEAD_DIM:]

    return jax.shard_map(
        layer_block,
        mesh=mesh,
        in_specs=(row_spec, P(("rep", "sp")), P(None), P(None, "tp"), P(None, "tp"), P(None, "tp"), P("tp", None), P(None, "tp"), P(None, "tp"), P("tp", None)),
        out_specs=(row_spec, cache_spec, cache_spec),
        check_vma=False,
    )
```

```python
import functools

import jax
import jax.numpy as jnp
from jax import lax
from jax.experimental import pallas as pl
from jax.experimental.pallas import tpu as pltpu
from jax.sharding import PartitionSpec as P

HEAD_DIM = 128
EPS = 1e-6
ROPE_BASE = 500000.0
EXP2_SCALE = HEAD_DIM ** -0.5 * 1.4426950408889634
MESH = pl.DeviceIdType.MESH
F32 = jnp.float32
BF16 = jnp.bfloat16

SLOTS = 4
SENDS = 4
HOP = 6
BACK_HOP = 8
DOWN_SLOTS = 2
RATE = 5, 13


def block_of(size, most):
    return most if size % most == 0 else most // 2


def odd(x):
    return x & 1


def below(n):
    return n - 1


def over(x, d):
    if d & (d - 1) == 0:
        return lax.shift_right_logical(x, d.bit_length() - 1)
    return lax.shift_right_logical(x * (65536 // d + 1), 16)


def rope_tables(positions):
    inv_freq = ROPE_BASE ** (-(jnp.arange(HEAD_DIM // 2, dtype=F32) * (2.0 / HEAD_DIM)))
    angles = positions.astype(F32)[:, None] * jnp.concatenate([inv_freq, inv_freq])[None, :]
    sign = jnp.where(jnp.arange(HEAD_DIM) < HEAD_DIM // 2, -1.0, 1.0)
    return jnp.cos(angles), jnp.sin(angles) * sign[None, :]


def rotate(vectors, cos_tab, sin_tab):
    return (vectors * cos_tab + pltpu.roll(vectors, HEAD_DIM // 2, 1) * sin_tab).astype(BF16)


def silu_mul(gate, up):
    return (gate / (1.0 + jnp.exp(-gate)) * up).astype(BF16)


def qkv_kernel(core_ref, x_ref, gain_ref, cos_ref, sin_ref, wk_ref, wv_ref, wq_ref, u_ref, kv_ref, vt_ref, q_other_ref, q_mine_ref, u_buf, inv_buf, wq_buf, wq_sem):
    phase, block = pl.program_id(0), pl.program_id(1)
    rows = x_ref.shape[0]
    at = pl.ds(pl.multiple_of(block * rows, rows), rows)
    q_cols = wq_buf.shape[2]
    core = core_ref[0]

    def weights(i):
        group = jnp.where(i == 0, 1 - core, core)
        return pltpu.make_async_copy(wq_ref.at[:, pl.ds(pl.multiple_of(group * q_cols, q_cols), q_cols)], wq_buf.at[i], wq_sem.at[i])

    @pl.when((phase == 0) & (block == 0))
    def _():
        weights(0).start()
        weights(1).start()

    @pl.when(phase == 0)
    def _():
        step = 16
        model = x_ref.shape[1]

        def squares(i, carry):
            part = pl.ds(pl.multiple_of(i * step, step), step)
            total = jnp.zeros((step, 128), F32)
            for j in range(model // 128):
                x = x_ref[part, j * 128:(j + 1) * 128].astype(F32)
                total = total + x * x
            inv_buf[part, :] = total
            return carry

        lax.fori_loop(0, rows // step, squares, 0, unroll=2)
        mean = jnp.sum(inv_buf[...], axis=1, keepdims=True) * (1.0 / model)
        inv_buf[...] = jnp.broadcast_to(lax.rsqrt(mean + EPS), inv_buf.shape)

        def scale(i, carry):
            part = pl.ds(pl.multiple_of(i * step, step), step)
            inv = inv_buf[part, :]
            for j in range(model // 128):
                cols = slice(j * 128, (j + 1) * 128)
                u = (x_ref[part, cols].astype(F32) * inv * gain_ref[:, cols]).astype(BF16)
                u_ref[part, cols] = u
                u_buf[pl.ds(pl.multiple_of(block * rows + i * step, step), step), cols] = u
            return carry

        lax.fori_loop(0, rows // step, scale, 0, unroll=2)
        k = jnp.dot(u_ref[...], wk_ref[...], preferred_element_type=F32)
        v = jnp.dot(u_ref[...], wv_ref[...], preferred_element_type=F32)
        for head in range(2):
            cols = slice(head * HEAD_DIM, (head + 1) * HEAD_DIM)
            kv_ref[head, :, :HEAD_DIM] = rotate(k[:, cols], cos_ref[at, :], sin_ref[at, :])
            kv_ref[head, :, HEAD_DIM:] = v[:, cols].astype(BF16)
            vt_ref[head] = v[:, cols].T.astype(BF16)

    def queries(q_ref, i):
        pl.when(block == 0)(lambda: weights(i).wait())
        q = jnp.dot(u_buf[at, :], wq_buf[i], preferred_element_type=F32)
        for head in range(q.shape[1] // HEAD_DIM):
            cols = slice(head * HEAD_DIM, (head + 1) * HEAD_DIM)
            q_ref[:, cols] = rotate(q[:, cols], cos_ref[at, :], sin_ref[at, :])

    pl.when(phase == 1)(lambda: queries(q_other_ref, 0))
    pl.when(phase == 2)(lambda: queries(q_mine_ref, 1))


def project(core, x_in, gain, cos_tab, sin_tab, w_k, w_v, w_q):
    tokens, model = x_in.shape
    rows = min(256, tokens // 2)
    blocks = tokens // rows
    q_cols = w_q.shape[1] // 2
    last = blocks - 1

    def first(p, i):
        return jnp.where(p == 0, i, last)

    return pl.pallas_call(
        qkv_kernel,
        grid_spec=pltpu.PrefetchScalarGridSpec(
            num_scalar_prefetch=1,
            grid=(3, blocks),
            in_specs=[
                pl.BlockSpec((rows, model), lambda p, i, c: (first(p, i), 0)),
                pl.BlockSpec((1, model), lambda p, i, c: (0, 0)),
                pl.BlockSpec((tokens, HEAD_DIM), lambda p, i, c: (0, 0)),
                pl.BlockSpec((tokens, HEAD_DIM), lambda p, i, c: (0, 0)),
                pl.BlockSpec((model, 2 * HEAD_DIM), lambda p, i, c: (0, 0)),
                pl.BlockSpec((model, 2 * HEAD_DIM), lambda p, i, c: (0, 0)),
                pl.BlockSpec(memory_space=pl.ANY),
            ],
            out_specs=[
                pl.BlockSpec((rows, model), lambda p, i, c: (first(p, i), 0)),
                pl.BlockSpec((2, rows, 2 * HEAD_DIM), lambda p, i, c: (0, first(p, i), 0)),
                pl.BlockSpec((2, HEAD_DIM, rows), lambda p, i, c: (0, 0, first(p, i))),
                pl.BlockSpec((rows, q_cols), lambda p, i, c: (jnp.where(p == 0, 0, jnp.where(p == 1, i, last)), 0)),
                pl.BlockSpec((rows, q_cols), lambda p, i, c: (jnp.where(p == 2, i, 0), 0)),
            ],
            scratch_shapes=[pltpu.VMEM((tokens, model), BF16), pltpu.VMEM((rows, 128), F32), pltpu.VMEM((2, model, q_cols), BF16), pltpu.SemaphoreType.DMA((2,))],
        ),
        out_shape=[
            jax.ShapeDtypeStruct((tokens, model), BF16),
            jax.ShapeDtypeStruct((2, tokens, 2 * HEAD_DIM), BF16),
            jax.ShapeDtypeStruct((2, HEAD_DIM, tokens), BF16),
            jax.ShapeDtypeStruct((tokens, q_cols), BF16),
            jax.ShapeDtypeStruct((tokens, q_cols), BF16),
        ],
        compiler_params=pltpu.CompilerParams(vmem_limit_bytes=60 * 2 ** 20),
        cost_estimate=pl.CostEstimate(flops=2 * tokens * model * (2 * q_cols + 4 * HEAD_DIM), bytes_accessed=6 * tokens * model, transcendentals=0),
        name="project",
    )(core, x_in, gain, cos_tab, sin_tab, w_k, w_v, w_q)


def layer_kernel(
    rows, att, keys_step,
    u_own, x_own, x_par, gain_ref, q_mine, q_other, kv, vt, w_gate, w_up, w_down, w_o,
    y_out, cache, u_par,
    wgu_buf, wd_buf, wo_buf, ubuf, hbuf, abuf, qbuf, kbuf, vtbuf, pbuf, rbuf, xbuf, ybuf, m_buf, l_buf, acc_buf, s0_buf, s1_buf, top_buf,
    wgu_sem, wd_sem, wo_sem, u_sem, near_sem, u_send, u_recv, q_send, q_recv, kv_send, kv_recv,
    h_send, h_recv, a_send, a_recv, lend_send, lend_recv, rs_send, rs_recv, x_sem, y_near, y_far, ag_recv, ag_send, credit,
):
    tokens, model = u_own.shape
    units = tokens // rows
    ff_half = w_gate.shape[1] // 2
    cols_half = model // 2
    bg = wgu_buf.shape[2] // 2
    wb = wd_buf.shape[2]
    bw = wb // 2
    nbg = ff_half // bg
    nbw = cols_half // bw
    q_cols = q_mine.shape[1]
    heads = q_cols // HEAD_DIM
    subs = rows // att
    per_unit = 2 * nbw
    pieces = per_unit * units
    unit_ticks = 2 * nbg + 2 * subs + 2 * nbw
    lent = below(units)

    z = lax.axis_index("tp")
    nz = lax.axis_size("tp")
    end = below(nz)
    sp = lax.axis_index("sp")
    core = sp % 2
    row_y = sp // 2
    twin = 1 - core
    partner = sp + twin - core
    other_y = 1 - row_y
    across = 2 * other_y + core
    across_partner = 2 * other_y + twin
    step_z = 1 - 2 * core
    hop = jnp.where(core == 0, z, end - z)
    z_next = jnp.clip(z + step_z, 0, end)
    z_prev = jnp.clip(z - step_z, 0, end)

    def mult(value, of):
        return pl.multiple_of(value, of)

    def gate_up_copies(n):
        cols = pl.ds(mult(core * ff_half + n * bg, bg), bg)
        slot = odd(n)
        return (
            pltpu.make_async_copy(w_gate.at[:, cols], wgu_buf.at[slot, :, pl.ds(0, bg)], wgu_sem.at[slot, 0]),
            pltpu.make_async_copy(w_up.at[:, cols], wgu_buf.at[slot, :, pl.ds(bg, bg)], wgu_sem.at[slot, 1]),
        )

    def start_gate_up(n):
        for copy in gate_up_copies(n):
            copy.start()

    def down_copy(n):
        b, k = n // 2, n % 2
        half = jnp.where(k == 0, core, twin)
        src = w_down.at[pl.ds(mult(half * ff_half, ff_half), ff_half), pl.ds(mult(core * cols_half + b * wb, wb), wb)]
        slot = n % DOWN_SLOTS
        return pltpu.make_async_copy(src, wd_buf.at[slot], wd_sem.at[slot])

    def out_copy(b):
        return pltpu.make_async_copy(w_o.at[:, pl.ds(mult(core * cols_half + b * wb, wb), wb)], wo_buf.at[odd(b)], wo_sem.at[odd(b)])

    def u_rows(u):
        return pl.ds(mult(u * rows, rows), rows)

    def own_u_copy(u):
        return pltpu.make_async_copy(u_own.at[u_rows(u), :], ubuf.at[u_rows(core), :], u_sem.at[0])

    def par_u_copy(u):
        return pltpu.make_async_copy(u_par.at[u_rows(u), :], ubuf.at[u_rows(twin), :], u_sem.at[1])

    def par_x_copy():
        return pltpu.make_async_copy(x_par.at[u_rows(0), :], ubuf.at[u_rows(twin), :], u_sem.at[1])

    def norm_par_rows():
        step = 16

        def body(i, carry):
            at = pl.ds(mult((twin) * rows + i * step, step), step)
            total = jnp.zeros((step, 128), F32)
            for j in range(model // 128):
                x = ubuf[at, j * 128:(j + 1) * 128].astype(F32)
                total = total + x * x
            inv = lax.rsqrt(jnp.sum(total, axis=1, keepdims=True) * (1.0 / model) + EPS)
            for j in range(model // 128):
                cols = slice(j * 128, (j + 1) * 128)
                ubuf[at, cols] = (ubuf[at, cols].astype(F32) * inv * gain_ref[:, cols]).astype(BF16)
            return carry

        lax.fori_loop(0, rows // step, body, 0, unroll=2 if rows % (2 * step) == 0 else 1)

    all_tokens = pl.ds(0, tokens)

    own_tokens = pl.ds(mult(sp * tokens, tokens), tokens)

    def own_copies():
        return (
            pltpu.make_async_copy(q_mine, qbuf.at[core, all_tokens, :], near_sem.at[0]),
            pltpu.make_async_copy(kv.at[core, :, pl.ds(0, HEAD_DIM)], kbuf.at[own_tokens, :], near_sem.at[1]),
            pltpu.make_async_copy(vt.at[core], vtbuf.at[:, own_tokens], near_sem.at[2]),
        )

    def own_cache():
        return pltpu.make_async_copy(kv.at[row_y], cache.at[own_tokens, :], near_sem.at[3])

    def h_copy(u, j):
        view = hbuf.at[odd(u), :, pl.ds(mult(core * ff_half + j * bg, bg), bg)]
        return pltpu.make_async_remote_copy(view, view, h_send.at[j], h_recv.at[odd(u), j], device_id={"sp": partner}, device_id_type=MESH)

    def far_u_copy(u):
        return pltpu.make_async_remote_copy(
            u_own.at[u_rows(u), :], u_par.at[u_rows(u), :], u_send.at[u], u_recv.at[u], device_id={"sp": partner}, device_id_type=MESH)

    def q_copy():
        return pltpu.make_async_remote_copy(q_other, qbuf.at[core, all_tokens, :], q_send, q_recv, device_id={"sp": partner}, device_id_type=MESH)

    peers = ((partner, twin, row_y), (across, core, other_y), (across_partner, twin, other_y))

    def key_copies(d):
        to, head, _ = peers[d]
        return (
            pltpu.make_async_remote_copy(
                kv.at[head, :, pl.ds(0, HEAD_DIM)], kbuf.at[own_tokens, :], kv_send.at[0, d], kv_recv.at[0, d], device_id={"sp": to}, device_id_type=MESH),
            pltpu.make_async_remote_copy(
                vt.at[head], vtbuf.at[:, own_tokens], kv_send.at[1, d], kv_recv.at[1, d], device_id={"sp": to}, device_id_type=MESH),
        )

    def cache_copy(d):
        to, _, head = peers[d]
        return pltpu.make_async_remote_copy(
            kv.at[head], cache.at[own_tokens, :], kv_send.at[2, d], kv_recv.at[2, d], device_id={"sp": to}, device_id_type=MESH)

    def a_copy(u):
        view = abuf.at[odd(u), :, pl.ds(mult(core * q_cols, q_cols), q_cols)]
        return pltpu.make_async_remote_copy(view, view, a_send, a_recv.at[odd(u)], device_id={"sp": partner}, device_id_type=MESH)

    def lend_copies():
        rows_there = pl.ds(tokens, rows)
        return tuple(
            pltpu.make_async_remote_copy(
                src.at[u_rows(lent), :], qbuf.at[core, rows_there, :], lend_send.at[0, d], lend_recv.at[0, d], device_id={"sp": to}, device_id_type=MESH)
            for d, (src, to) in enumerate(((q_mine, across), (q_other, across_partner)))
        )

    def lent_copies():
        view = abuf.at[2, :, pl.ds(mult(core * q_cols, q_cols), q_cols)]
        return tuple(
            pltpu.make_async_remote_copy(view, view, lend_send.at[1, d], lend_recv.at[1, d], device_id={"sp": to}, device_id_type=MESH)
            for d, to in enumerate((across, across_partner))
        )

    def part(p):
        u = over(p, per_unit)
        i = p - u * per_unit
        return u, lax.shift_right_logical(i, 1), odd(i)

    def sum_view(p):
        u, b, r = part(p)
        return pbuf.at[odd(u), pl.ds(mult(r * rows, rows), rows), pl.ds(mult(b * bw, bw), bw)]

    def sum_copy(p):
        return pltpu.make_async_remote_copy(
            sum_view(p), rbuf.at[p & (SLOTS - 1)], rs_send.at[p & (SENDS - 1)], rs_recv.at[p & (SLOTS - 1)], device_id={"tp": z_next}, device_id_type=MESH)

    def y_view(owner, p):
        u, b, _ = part(p)
        return y_out.at[pl.ds(mult(u * rows, rows), rows), pl.ds(mult(owner * cols_half + b * bw, bw), bw)]

    def start_x(p):
        u, b, r = part(p)
        src = (pl.ds(mult(u * rows, rows), rows), pl.ds(mult(core * cols_half + b * bw, bw), bw))

        @pl.when(r == core)
        def _():
            pltpu.make_async_copy(x_own.at[src[0], src[1]], xbuf.at[odd(p)], x_sem.at[odd(p)]).start()

        @pl.when(r != core)
        def _():
            pltpu.make_async_copy(x_par.at[src[0], src[1]], xbuf.at[odd(p)], x_sem.at[odd(p)]).start()

    def near_local(p):
        return pltpu.make_async_copy(ybuf.at[p & (SENDS - 1)], y_view(core, p), y_near.at[p & (SENDS - 1)])

    def near_remote(p):
        return pltpu.make_async_remote_copy(
            ybuf.at[p & (SENDS - 1)], y_view(core, p), y_near.at[p & (SENDS - 1)], ag_recv.at[core, lax.shift_right_logical(p, 1)], device_id={"sp": partner}, device_id_type=MESH)

    def far_remote(p):
        _, _, r = part(p)
        return pltpu.make_async_remote_copy(
            ybuf.at[p & (SENDS - 1)], y_view(core, p), y_far.at[p & (SENDS - 1)], ag_recv.at[core, lax.shift_right_logical(p, 1)],
            device_id={"tp": z_prev, "sp": 2 * row_y + r}, device_id_type=MESH)

    def wait_result_out(p):
        near_local(p).wait()
        far_remote(p).wait_send()

    def back_copy(owner, q):
        view = y_view(owner, 2 * q)
        z_to = jnp.clip(z - 1 + 2 * owner, 0, end)
        return pltpu.make_async_remote_copy(view, view, ag_send.at[owner, q], ag_recv.at[owner, q], device_id={"tp": z_to}, device_id_type=MESH)

    def sum_op(p):
        view = sum_view(p)

        @pl.when(hop > 0)
        def _():
            sum_copy(p).wait_recv()
            u, b, r = part(p)
            at = (odd(u), pl.ds(mult(r * rows, rows), rows), pl.ds(mult(b * bw, bw), bw))
            pbuf[at] = pbuf[at] + rbuf[p & (SLOTS - 1)]

            @pl.when(p + SLOTS < pieces)
            def _():
                pl.semaphore_signal(credit, inc=1, device_id={"tp": z_prev}, device_id_type=MESH)

        @pl.when(hop < end)
        def _():
            @pl.when(p >= SENDS)
            def _():
                sum_copy(p - SENDS).wait_send()

            @pl.when(p >= SLOTS)
            def _():
                pl.semaphore_wait(credit, 1)

            sum_copy(p).start()

        @pl.when(hop == end)
        def _():
            @pl.when(p >= SENDS)
            def _():
                wait_result_out(p - SENDS)

            slot = p & (SENDS - 1)
            pltpu.make_async_copy(x_own.at[pl.ds(0, rows), pl.ds(0, bw)], xbuf.at[odd(p)], x_sem.at[odd(p)]).wait()
            ybuf[slot] = (xbuf[odd(p)].astype(F32) + view[...]).astype(BF16)

            @pl.when(p + 2 < pieces)
            def _():
                start_x(p + 2)

            far_remote(p).start()
            r = odd(p)

            @pl.when(r == core)
            def _():
                near_local(p).start()

            @pl.when(r != core)
            def _():
                near_remote(p).start()

    def back_op(owner, q, distance):
        back_copy(owner, q).wait_recv()

        @pl.when((distance > 0) & (distance < end))
        def _():
            back_copy(owner, q).start()

    def ticks(t, count):
        def body(i, carry):
            tick(t + i)
            return carry

        lax.fori_loop(0, count, body, 0)

    many, span_of = RATE

    def piece_at(v, span, per):
        v_ok = jnp.maximum(v, 0)
        u = over(v_ok, span)
        w = v_ok - u * span
        i = over(many * w + span_of - 1, span_of)
        return u * per + i, (v >= 0) & (span_of * i - many * w < many) & (i < per) & (u < units)

    first_back = 7 + end * HOP

    def tick(t):
        p, here = piece_at(t - 3 - hop * HOP, unit_ticks, per_unit)

        @pl.when(here)
        def _():
            sum_op(p)

        owner = odd(t)
        distance = jnp.where(owner == 0, end - z, z)
        q, back = piece_at(lax.shift_right_arithmetic(t - first_back - distance * BACK_HOP, 1), unit_ticks // 2, nbw)

        @pl.when(back & ((distance > 0) | (core != owner)))
        def _():
            back_op(owner, q, distance)

    last_tick = below(units) * unit_ticks + 2 * (span_of * nbw // many + 1) + first_back + end * BACK_HOP + 2

    def attend(first, token, slot, r, s):
        q_rows = qbuf[r, pl.ds(mult(first, att), att), :]
        q_stack = jnp.concatenate([q_rows[:, i * HEAD_DIM:(i + 1) * HEAD_DIM] for i in range(heads)], axis=0)
        m_buf[...] = jnp.full_like(m_buf, -jnp.inf)
        l_buf[...] = jnp.zeros_like(l_buf)
        acc_buf[...] = jnp.zeros_like(acc_buf)

        def stage(held, held_start, fresh, fresh_start, masked=False):
            if fresh is not None:
                start = mult(fresh_start, keys_step)
                part = lax.dot_general(kbuf[pl.ds(start, keys_step), :], q_stack, (((1,), (1,)), ((), ())), preferred_element_type=F32)
                if masked:
                    key_id = start + lax.broadcasted_iota(jnp.int32, part.shape, 0)
                    token_id = token + (lax.broadcasted_iota(jnp.int32, part.shape, 1) & (att - 1))
                    part = jnp.where(key_id <= token_id, part, -jnp.inf)
                fresh[...] = part
                top = jnp.max(part.reshape(keys_step // 8, 8, part.shape[1]), axis=0)
            if held is not None:
                m_old = m_buf[...]
                m_new = jnp.maximum(m_old, jnp.max(top_buf[...], axis=0, keepdims=True))
                m_buf[...] = m_new
                fade = jnp.exp2((m_old - m_new) * EXP2_SCALE)
                w = jnp.exp2((held[...] - m_new[0:1]) * EXP2_SCALE)
                l_buf[...] = l_buf[...] * fade + jnp.sum(w.reshape(keys_step // 8, 8, w.shape[1]), axis=0)
                acc_buf[...] = acc_buf[...] * fade[0:1] + jnp.dot(
                    vtbuf[:, pl.ds(mult(held_start, keys_step), keys_step)], w.astype(BF16), preferred_element_type=F32)
            if fresh is not None:
                top_buf[...] = top

        clear = token // keys_step
        edge = clear * keys_step
        stage(None, None, s0_buf, edge, True)

        def pair(i, carry):
            stage(s0_buf, jnp.where(i == 0, edge, (2 * i - 1) * keys_step), s1_buf, 2 * i * keys_step)
            stage(s1_buf, 2 * i * keys_step, s0_buf, (2 * i + 1) * keys_step)
            return carry

        pairs = clear // 2
        lax.fori_loop(0, pairs, pair, 0)
        held = jnp.where(pairs == 0, edge, (2 * pairs - 1) * keys_step)

        @pl.when(clear % 2 == 1)
        def _():
            stage(s0_buf, held, s1_buf, (clear - 1) * keys_step)
            stage(s1_buf, (clear - 1) * keys_step, None, None)

        @pl.when(clear % 2 == 0)
        def _():
            stage(s0_buf, held, None, None)

        out = (acc_buf[...] / jnp.sum(l_buf[...], axis=0, keepdims=True)).astype(BF16)
        for i in range(heads):
            abuf[slot, pl.ds(mult(r * rows + s * att, att), att), pl.ds(mult(core * q_cols + i * HEAD_DIM, HEAD_DIM), HEAD_DIM)] = out[:, i * att:(i + 1) * att].T

    start_gate_up(0)
    par_x_copy().start()
    own_u_copy(0).start()
    start_gate_up(1)
    for copy in own_copies():
        copy.start()
    own_cache().start()

    @pl.when(hop == end)
    def _():
        start_x(0)
        start_x(1)

    barrier = pltpu.get_barrier_semaphore()
    for other in (partner, across, across_partner):
        pl.semaphore_signal(barrier, inc=1, device_id={"sp": other}, device_id_type=MESH)

    @pl.when(z > 0)
    def _():
        pl.semaphore_signal(barrier, inc=1, device_id={"tp": z - 1}, device_id_type=MESH)
        pl.semaphore_signal(barrier, inc=1, device_id={"tp": z - 1, "sp": partner}, device_id_type=MESH)

    @pl.when(z < end)
    def _():
        pl.semaphore_signal(barrier, inc=1, device_id={"tp": z + 1}, device_id_type=MESH)
        pl.semaphore_signal(barrier, inc=1, device_id={"tp": z + 1, "sp": partner}, device_id_type=MESH)

    par_x_copy().wait()
    norm_par_rows()
    pl.semaphore_wait(barrier, 3 + 2 * (z > 0).astype(jnp.int32) + 2 * (z < end).astype(jnp.int32))

    for d in (1, 2, 0):
        for copy in key_copies(d):
            copy.start()
    q_copy().start()

    @pl.when(row_y == 1)
    def _():
        for copy in lend_copies():
            copy.start()

    def send_u(u, carry):
        far_u_copy(u).start()
        return carry

    lax.fori_loop(1, units, send_u, 0)

    def unit(u, carry):
        t0 = u * unit_ticks
        gate_up_tick = t0 - 2 * nbg - 2 * subs
        own_u_copy(u).wait()

        @pl.when(u > 0)
        def _():
            par_u_copy(u).wait()

        for n in range(DOWN_SLOTS):
            down_copy(n).start()
        out_copy(0).start()
        out_copy(1).start()

        def gate_up(n, carry):
            slot = odd(n)
            copy_g, copy_u = gate_up_copies(n)
            copy_g.wait()
            copy_u.wait()
            both = jnp.dot(ubuf[...], wgu_buf[slot], preferred_element_type=F32)
            hbuf[odd(u), :, pl.ds(mult(core * ff_half + n * bg, bg), bg)] = silu_mul(both[:, :bg], both[:, bg:])

            @pl.when(n + 2 < nbg)
            def _():
                start_gate_up(n + 2)

            ticks(gate_up_tick + 2 * n, 2)
            h_copy(u, n).start()
            return carry

        lax.fori_loop(0, nbg, gate_up, 0)

        @pl.when(u == 0)
        def _():
            for copy in own_copies():
                copy.wait()
            for d in range(3):
                for copy in key_copies(d):
                    copy.wait()
            q_copy().wait()
            for d in range(3):
                cache_copy(d).start()

        borrows = (row_y == 0) & (u == lent - 1)
        lends = (row_y == 1) & (u == lent)
        a_slot = jnp.where(lends, 2, odd(u))

        @pl.when(borrows)
        def _():
            for copy in lend_copies():
                copy.wait_recv()

        def sub(i, carry):
            mine = i < 2 * subs
            j = jnp.where(mine, i, i - 2 * subs)
            r = over(j, subs)
            part = j - r * subs
            first = jnp.where(mine, u * rows, tokens) + part * att
            token = jnp.where(mine, (2 * row_y + r) * tokens + u * rows, (2 + r) * tokens + lent * rows) + part * att
            attend(first, token, jnp.where(mine, odd(u), 2), r, part)
            ticks(t0 - 2 * subs + i, mine.astype(jnp.int32))
            return carry

        lax.fori_loop(0, jnp.where(lends, 0, jnp.where(borrows, 4 * subs, 2 * subs)), sub, 0)

        @pl.when(lends)
        def _():
            ticks(t0 - 2 * subs, 2 * subs)

        @pl.when(jnp.logical_not(lends))
        def _():
            a_copy(u).start()

        @pl.when(borrows)
        def _():
            for copy in lent_copies():
                copy.start()

        @pl.when(u + 1 < units)
        def _():
            own_u_copy(u + 1).start()
            far_u_copy(u + 1).wait()
            par_u_copy(u + 1).start()
            start_gate_up(0)
            start_gate_up(1)

        def wait_h(j, carry):
            h_copy(u, j).wait()
            return carry

        def down(b, carry):
            cols = pl.ds(mult(b * wb, wb), wb)
            own_rows = pl.ds(mult(core * ff_half, ff_half), ff_half)
            par_rows = pl.ds(mult((twin) * ff_half, ff_half), ff_half)
            down_copy(2 * b).wait()
            pbuf[odd(u), :, cols] = jnp.dot(hbuf[odd(u), :, own_rows], wd_buf[0], preferred_element_type=F32)

            @pl.when(b + 1 < nbw // 2)
            def _():
                down_copy(2 * b + 2).start()

            ticks(t0 + 4 * b, 2)

            @pl.when(b == 0)
            def _():
                lax.fori_loop(0, nbg, wait_h, 0)

                @pl.when(lends)
                def _():
                    for copy in lent_copies():
                        copy.wait_recv()

                @pl.when(jnp.logical_not(lends))
                def _():
                    a_copy(u).wait()

            down_copy(2 * b + 1).wait()
            out_copy(b).wait()
            pbuf[odd(u), :, cols] = (
                pbuf[odd(u), :, cols]
                + jnp.dot(hbuf[odd(u), :, par_rows], wd_buf[1], preferred_element_type=F32)
                + jnp.dot(abuf[a_slot], wo_buf[odd(b)], preferred_element_type=F32)
            )

            @pl.when(b + 1 < nbw // 2)
            def _():
                down_copy(2 * b + 3).start()

            @pl.when(b + 2 < nbw // 2)
            def _():
                out_copy(b + 2).start()

            ticks(t0 + 4 * b + 2, 2)
            return carry

        lax.fori_loop(0, nbw // 2, down, 0)
        return carry

    lax.fori_loop(0, units, unit, 0)

    def drain(t, carry):
        tick(t)
        return carry

    lax.fori_loop(below(units) * unit_ticks + 2 * nbw, last_tick + 1, drain, 0)

    def sums_out(i, carry):
        p = pieces - SENDS + i

        @pl.when(hop < end)
        def _():
            sum_copy(p).wait_send()

        @pl.when(hop == end)
        def _():
            wait_result_out(p)

        return carry

    lax.fori_loop(0, SENDS, sums_out, 0)

    for owner in (0, 1):
        distance = end - z if owner == 0 else z

        @pl.when((distance > 0) & (distance < end))
        def _():
            def backs_out(q, carry):
                back_copy(owner, q).wait_send()
                return carry

            lax.fori_loop(0, pieces // 2, backs_out, 0)

    own_cache().wait()
    for d in range(3):
        cache_copy(d).wait()

    @pl.when(row_y == 1)
    def _():
        for copy in lend_copies():
            copy.wait_send()

    @pl.when(row_y == 0)
    def _():
        for copy in lent_copies():
            copy.wait_send()


def layer(u_own, x_own, x_par, gain, q_mine, q_other, kv, vt, w_gate, w_up, w_down, w_o):
    tokens, model = u_own.shape
    ff = w_gate.shape[1]
    ff_half, cols_half = ff // 2, model // 2
    rows = tokens // 4
    att = min(128, rows)
    bg, bw = block_of(ff_half, 256), block_of(cols_half, 512) // 2
    wb = 2 * bw
    nbg, nbw = ff_half // bg, cols_half // bw
    q_cols = q_mine.shape[1]
    kv_tokens = 4 * tokens
    keys_step = min(512, kv_tokens // 4)
    units = tokens // rows
    pieces = 2 * nbw * units
    stack = att * (q_cols // HEAD_DIM)
    any_spec = pl.BlockSpec(memory_space=pl.ANY)
    dma = pltpu.SemaphoreType.DMA
    two, sends, quad, peer = dma((2,)), dma((SENDS,)), dma((2, 2)), dma((3, 3))
    macs = tokens * model * (3 * ff + w_o.shape[0])
    y_out, cache, _ = pl.pallas_call(
        functools.partial(layer_kernel, rows, att, keys_step),
        out_shape=[
            jax.ShapeDtypeStruct((tokens, model), BF16),
            jax.ShapeDtypeStruct((kv_tokens, 2 * HEAD_DIM), BF16),
            jax.ShapeDtypeStruct((tokens, model), BF16),
        ],
        in_specs=[any_spec] * 3 + [pl.BlockSpec(memory_space=pltpu.VMEM)] + [any_spec] * 8,
        out_specs=[any_spec] * 3,
        scratch_shapes=[
            pltpu.VMEM((2, model, 2 * bg), BF16),
            pltpu.VMEM((DOWN_SLOTS, ff_half, wb), BF16),
            pltpu.VMEM((2, w_o.shape[0], wb), BF16),
            pltpu.VMEM((2 * rows, model), BF16),
            pltpu.VMEM((2, 2 * rows, ff), BF16),
            pltpu.VMEM((3, 2 * rows, w_o.shape[0]), BF16),
            pltpu.VMEM((2, tokens + rows, q_cols), BF16),
            pltpu.VMEM((kv_tokens, HEAD_DIM), BF16),
            pltpu.VMEM((HEAD_DIM, kv_tokens), BF16),
            pltpu.VMEM((2, 2 * rows, cols_half), F32),
            pltpu.VMEM((SLOTS, rows, bw), F32),
            pltpu.VMEM((2, rows, bw), BF16),
            pltpu.VMEM((SENDS, rows, bw), BF16),
            pltpu.VMEM((8, stack), F32),
            pltpu.VMEM((8, stack), F32),
            pltpu.VMEM((HEAD_DIM, stack), F32),
            pltpu.VMEM((keys_step, stack), F32),
            pltpu.VMEM((keys_step, stack), F32),
            pltpu.VMEM((8, stack), F32),
            quad, dma((DOWN_SLOTS,)), two, two, dma((4,)), dma((units,)), dma((units,)), dma, dma, peer, peer,
            dma((nbg,)), dma((2, nbg)), dma, two, quad, quad,
            sends, dma((SLOTS,)), sends, sends, sends,
            dma((2, pieces // 2)), dma((2, pieces // 2)),
            pltpu.SemaphoreType.REGULAR,
        ],
        compiler_params=pltpu.CompilerParams(
            collective_id=0, has_side_effects=True, vmem_limit_bytes=67043328),
        cost_estimate=pl.CostEstimate(flops=macs, bytes_accessed=6 * ff_half * model * units, transcendentals=0),
        name="layer",
    )(u_own, x_own, x_par, gain, q_mine, q_other, kv, vt, w_gate, w_up, w_down, w_o)
    return y_out, cache


def solution(mesh):
    row_spec = P(("rep", "sp"), None)
    cache_spec = P("rep", ("tp", "sp"), None)
    other_core = [(0, 1), (1, 0), (2, 3), (3, 2)]

    def layer_block(x_in, positions, norm_gain, w_q, w_k, w_v, w_o, w_gate, w_up, w_down):
        core = (lax.axis_index("sp") % 2).astype(jnp.int32).reshape(1)
        x_par = lax.ppermute(x_in, "sp", other_core)
        cos_tab, sin_tab = rope_tables(positions)
        gain = norm_gain.reshape(1, -1)
        normed, kv, vt, q_other, q_mine = project(core, x_in, gain, cos_tab, sin_tab, w_k, w_v, w_q)
        y_out, cache = layer(normed, x_in, x_par, gain, q_mine, q_other, kv, vt, w_gate, w_up, w_down, w_o)
        return y_out, cache[:, None, :HEAD_DIM], cache[:, None, HEAD_DIM:]

    return jax.shard_map(
        layer_block,
        mesh=mesh,
        in_specs=(row_spec, P(("rep", "sp")), P(None), P(None, "tp"), P(None, "tp"), P(None, "tp"), P("tp", None), P(None, "tp"), P(None, "tp"), P("tp", None)),
        out_specs=(row_spec, cache_spec, cache_spec),
        check_vma=False,
    )
```

```python
import functools

import jax
import jax.numpy as jnp
from jax import lax
from jax.experimental import pallas as pl
from jax.experimental.pallas import tpu as pltpu
from jax.sharding import PartitionSpec as P

HEAD_DIM = 128
EPS = 1e-6
ROPE_BASE = 500000.0
EXP2_SCALE = HEAD_DIM ** -0.5 * 1.4426950408889634
MESH = pl.DeviceIdType.MESH
F32 = jnp.float32
BF16 = jnp.bfloat16

SLOTS = 4
SENDS = 4
HOP = 7
BACK_HOP = 8
DOWN_SLOTS = 2
VMEM_BYTES = 67043328
RATE = 5, 13


def block_of(size, most):
    return most if size % most == 0 else most // 2


def odd(x):
    return x & 1


def below(n):
    return n - 1


def over(x, d):
    if d & (d - 1) == 0:
        return lax.shift_right_logical(x, d.bit_length() - 1)
    return lax.shift_right_logical(x * (65536 // d + 1), 16)


def rope_tables(positions):
    inv_freq = ROPE_BASE ** (-(jnp.arange(HEAD_DIM // 2, dtype=F32) * (2.0 / HEAD_DIM)))
    angles = positions.astype(F32)[:, None] * jnp.concatenate([inv_freq, inv_freq])[None, :]
    sign = jnp.where(jnp.arange(HEAD_DIM) < HEAD_DIM // 2, -1.0, 1.0)
    return jnp.cos(angles), jnp.sin(angles) * sign[None, :]


def rotate(vectors, cos_tab, sin_tab):
    return (vectors * cos_tab + pltpu.roll(vectors, HEAD_DIM // 2, 1) * sin_tab).astype(BF16)


def silu_mul(gate, up):
    return (gate / (1.0 + jnp.exp(-gate)) * up).astype(BF16)


def qkv_kernel(core_ref, x_ref, gain_ref, cos_ref, sin_ref, wk_ref, wv_ref, wq_ref, u_ref, kv_ref, vt_ref, q_other_ref, q_mine_ref, u_buf, inv_buf, wq_buf, wq_sem):
    phase, block = pl.program_id(0), pl.program_id(1)
    rows = x_ref.shape[0]
    at = pl.ds(pl.multiple_of(block * rows, rows), rows)
    q_cols = wq_buf.shape[2]
    core = core_ref[0]

    def weights(i):
        group = jnp.where(i == 0, 1 - core, core)
        return pltpu.make_async_copy(wq_ref.at[:, pl.ds(pl.multiple_of(group * q_cols, q_cols), q_cols)], wq_buf.at[i], wq_sem.at[i])

    @pl.when((phase == 0) & (block == 0))
    def _():
        weights(0).start()
        weights(1).start()

    @pl.when(phase == 0)
    def _():
        step = 16
        model = x_ref.shape[1]

        def squares(i, carry):
            part = pl.ds(pl.multiple_of(i * step, step), step)
            total = jnp.zeros((step, 128), F32)
            for j in range(model // 128):
                x = x_ref[part, j * 128:(j + 1) * 128].astype(F32)
                total = total + x * x
            inv_buf[part, :] = total
            return carry

        lax.fori_loop(0, rows // step, squares, 0, unroll=4)
        mean = jnp.sum(inv_buf[...], axis=1, keepdims=True) * (1.0 / model)
        inv_buf[...] = jnp.broadcast_to(lax.rsqrt(mean + EPS), inv_buf.shape)

        def scale(i, carry):
            part = pl.ds(pl.multiple_of(i * step, step), step)
            inv = inv_buf[part, :]
            for j in range(model // 128):
                cols = slice(j * 128, (j + 1) * 128)
                u = (x_ref[part, cols].astype(F32) * inv * gain_ref[:, cols]).astype(BF16)
                u_ref[part, cols] = u
                u_buf[pl.ds(pl.multiple_of(block * rows + i * step, step), step), cols] = u
            return carry

        lax.fori_loop(0, rows // step, scale, 0, unroll=4)
        k = jnp.dot(u_ref[...], wk_ref[...], preferred_element_type=F32)
        v = jnp.dot(u_ref[...], wv_ref[...], preferred_element_type=F32)
        for head in range(2):
            cols = slice(head * HEAD_DIM, (head + 1) * HEAD_DIM)
            kv_ref[head, :, :HEAD_DIM] = rotate(k[:, cols], cos_ref[at, :], sin_ref[at, :])
            kv_ref[head, :, HEAD_DIM:] = v[:, cols].astype(BF16)
            vt_ref[head] = v[:, cols].T.astype(BF16)

    def queries(q_ref, i):
        pl.when(block == 0)(lambda: weights(i).wait())
        q = jnp.dot(u_buf[at, :], wq_buf[i], preferred_element_type=F32)
        for head in range(q.shape[1] // HEAD_DIM):
            cols = slice(head * HEAD_DIM, (head + 1) * HEAD_DIM)
            q_ref[:, cols] = rotate(q[:, cols], cos_ref[at, :], sin_ref[at, :])

    pl.when(phase == 1)(lambda: queries(q_other_ref, 0))
    pl.when(phase == 2)(lambda: queries(q_mine_ref, 1))


def project(core, x_in, gain, cos_tab, sin_tab, w_k, w_v, w_q):
    tokens, model = x_in.shape
    rows = min(256, tokens // 2)
    blocks = tokens // rows
    q_cols = w_q.shape[1] // 2
    last = blocks - 1

    def first(p, i):
        return jnp.where(p == 0, i, last)

    return pl.pallas_call(
        qkv_kernel,
        grid_spec=pltpu.PrefetchScalarGridSpec(
            num_scalar_prefetch=1,
            grid=(3, blocks),
            in_specs=[
                pl.BlockSpec((rows, model), lambda p, i, c: (first(p, i), 0)),
                pl.BlockSpec((1, model), lambda p, i, c: (0, 0)),
                pl.BlockSpec((tokens, HEAD_DIM), lambda p, i, c: (0, 0)),
                pl.BlockSpec((tokens, HEAD_DIM), lambda p, i, c: (0, 0)),
                pl.BlockSpec((model, 2 * HEAD_DIM), lambda p, i, c: (0, 0)),
                pl.BlockSpec((model, 2 * HEAD_DIM), lambda p, i, c: (0, 0)),
                pl.BlockSpec(memory_space=pl.ANY),
            ],
            out_specs=[
                pl.BlockSpec((rows, model), lambda p, i, c: (first(p, i), 0)),
                pl.BlockSpec((2, rows, 2 * HEAD_DIM), lambda p, i, c: (0, first(p, i), 0)),
                pl.BlockSpec((2, HEAD_DIM, rows), lambda p, i, c: (0, 0, first(p, i))),
                pl.BlockSpec((rows, q_cols), lambda p, i, c: (jnp.where(p == 0, 0, jnp.where(p == 1, i, last)), 0)),
                pl.BlockSpec((rows, q_cols), lambda p, i, c: (jnp.where(p == 2, i, 0), 0)),
            ],
            scratch_shapes=[pltpu.VMEM((tokens, model), BF16), pltpu.VMEM((rows, 128), F32), pltpu.VMEM((2, model, q_cols), BF16), pltpu.SemaphoreType.DMA((2,))],
        ),
        out_shape=[
            jax.ShapeDtypeStruct((tokens, model), BF16),
            jax.ShapeDtypeStruct((2, tokens, 2 * HEAD_DIM), BF16),
            jax.ShapeDtypeStruct((2, HEAD_DIM, tokens), BF16),
            jax.ShapeDtypeStruct((tokens, q_cols), BF16),
            jax.ShapeDtypeStruct((tokens, q_cols), BF16),
        ],
        compiler_params=pltpu.CompilerParams(vmem_limit_bytes=VMEM_BYTES),
        cost_estimate=pl.CostEstimate(flops=2 * tokens * model * (2 * q_cols + 4 * HEAD_DIM), bytes_accessed=6 * tokens * model, transcendentals=0),
        name="project",
    )(core, x_in, gain, cos_tab, sin_tab, w_k, w_v, w_q)


def layer_kernel(
    rows, att, keys_step,
    u_own, x_own, x_par, gain_ref, q_mine, q_other, kv, vt, w_gate, w_up, w_down, w_o,
    y_out, cache, u_par,
    wgu_buf, wd_buf, wo_buf, ubuf, hbuf, abuf, qbuf, kbuf, vtbuf, pbuf, rbuf, xbuf, ybuf, m_buf, l_buf, acc_buf, s0_buf, s1_buf, top_buf,
    wgu_sem, wd_sem, wo_sem, u_sem, near_sem, u_send, u_recv, q_send, q_recv, kv_send, kv_recv,
    h_send, h_recv, a_send, a_recv, lend_send, lend_recv, rs_send, rs_recv, x_sem, y_near, y_far, ag_recv, ag_send, credit,
):
    tokens, model = u_own.shape
    units = tokens // rows
    ff_half = w_gate.shape[1] // 2
    cols_half = model // 2
    bg = wgu_buf.shape[2] // 2
    wb = wd_buf.shape[2]
    bw = wb // 2
    nbg = ff_half // bg
    nbw = cols_half // bw
    q_cols = q_mine.shape[1]
    heads = q_cols // HEAD_DIM
    subs = rows // att
    per_unit = 2 * nbw
    pieces = per_unit * units
    unit_ticks = 2 * nbg + 2 * subs + 2 * nbw
    lent = below(units)

    z = lax.axis_index("tp")
    nz = lax.axis_size("tp")
    end = below(nz)
    sp = lax.axis_index("sp")
    core = sp % 2
    row_y = sp // 2
    twin = 1 - core
    partner = sp + twin - core
    other_y = 1 - row_y
    across = 2 * other_y + core
    across_partner = 2 * other_y + twin
    step_z = 1 - 2 * core
    hop = jnp.where(core == 0, z, end - z)
    z_next = jnp.clip(z + step_z, 0, end)
    z_prev = jnp.clip(z - step_z, 0, end)

    def mult(value, of):
        return pl.multiple_of(value, of)

    def gate_up_copies(n):
        cols = pl.ds(mult(core * ff_half + n * bg, bg), bg)
        slot = odd(n)
        return (
            pltpu.make_async_copy(w_gate.at[:, cols], wgu_buf.at[slot, :, pl.ds(0, bg)], wgu_sem.at[slot, 0]),
            pltpu.make_async_copy(w_up.at[:, cols], wgu_buf.at[slot, :, pl.ds(bg, bg)], wgu_sem.at[slot, 1]),
        )

    def start_gate_up(n):
        for copy in gate_up_copies(n):
            copy.start()

    def down_copy(n):
        b, k = n // 2, n % 2
        half = jnp.where(k == 0, core, twin)
        src = w_down.at[pl.ds(mult(half * ff_half, ff_half), ff_half), pl.ds(mult(core * cols_half + b * wb, wb), wb)]
        slot = n % DOWN_SLOTS
        return pltpu.make_async_copy(src, wd_buf.at[slot], wd_sem.at[slot])

    def out_copy(b):
        return pltpu.make_async_copy(w_o.at[:, pl.ds(mult(core * cols_half + b * wb, wb), wb)], wo_buf.at[odd(b)], wo_sem.at[odd(b)])

    def u_rows(u):
        return pl.ds(mult(u * rows, rows), rows)

    def own_u_copy(u):
        return pltpu.make_async_copy(u_own.at[u_rows(u), :], ubuf.at[u_rows(core), :], u_sem.at[0])

    def par_u_copy(u):
        return pltpu.make_async_copy(u_par.at[u_rows(u), :], ubuf.at[u_rows(twin), :], u_sem.at[1])

    def par_x_copy():
        return pltpu.make_async_copy(x_par.at[u_rows(0), :], ubuf.at[u_rows(twin), :], u_sem.at[1])

    def norm_par_rows():
        step = 16

        def body(i, carry):
            at = pl.ds(mult((twin) * rows + i * step, step), step)
            total = jnp.zeros((step, 128), F32)
            for j in range(model // 128):
                x = ubuf[at, j * 128:(j + 1) * 128].astype(F32)
                total = total + x * x
            inv = lax.rsqrt(jnp.sum(total, axis=1, keepdims=True) * (1.0 / model) + EPS)
            for j in range(model // 128):
                cols = slice(j * 128, (j + 1) * 128)
                ubuf[at, cols] = (ubuf[at, cols].astype(F32) * inv * gain_ref[:, cols]).astype(BF16)
            return carry

        lax.fori_loop(0, rows // step, body, 0, unroll=4 if rows % (4 * step) == 0 else 1)

    all_tokens = pl.ds(0, tokens)

    own_tokens = pl.ds(mult(sp * tokens, tokens), tokens)

    def own_copies():
        return (
            pltpu.make_async_copy(q_mine, qbuf.at[core, all_tokens, :], near_sem.at[0]),
            pltpu.make_async_copy(kv.at[core, :, pl.ds(0, HEAD_DIM)], kbuf.at[own_tokens, :], near_sem.at[1]),
            pltpu.make_async_copy(vt.at[core], vtbuf.at[:, own_tokens], near_sem.at[2]),
        )

    def own_cache():
        return pltpu.make_async_copy(kv.at[row_y], cache.at[own_tokens, :], near_sem.at[3])

    def h_copy(u, j):
        view = hbuf.at[odd(u), :, pl.ds(mult(core * ff_half + j * bg, bg), bg)]
        return pltpu.make_async_remote_copy(view, view, h_send.at[j], h_recv.at[odd(u), j], device_id={"sp": partner}, device_id_type=MESH)

    def far_u_copy(u):
        return pltpu.make_async_remote_copy(
            u_own.at[u_rows(u), :], u_par.at[u_rows(u), :], u_send.at[u], u_recv.at[u], device_id={"sp": partner}, device_id_type=MESH)

    def q_copy():
        return pltpu.make_async_remote_copy(q_other, qbuf.at[core, all_tokens, :], q_send, q_recv, device_id={"sp": partner}, device_id_type=MESH)

    peers = ((partner, twin, row_y), (across, core, other_y), (across_partner, twin, other_y))

    def key_copies(d):
        to, head, _ = peers[d]
        return (
            pltpu.make_async_remote_copy(
                kv.at[head, :, pl.ds(0, HEAD_DIM)], kbuf.at[own_tokens, :], kv_send.at[0, d], kv_recv.at[0, d], device_id={"sp": to}, device_id_type=MESH),
            pltpu.make_async_remote_copy(
                vt.at[head], vtbuf.at[:, own_tokens], kv_send.at[1, d], kv_recv.at[1, d], device_id={"sp": to}, device_id_type=MESH),
        )

    def cache_copy(d):
        to, _, head = peers[d]
        return pltpu.make_async_remote_copy(
            kv.at[head], cache.at[own_tokens, :], kv_send.at[2, d], kv_recv.at[2, d], device_id={"sp": to}, device_id_type=MESH)

    def a_copy(u):
        view = abuf.at[odd(u), :, pl.ds(mult(core * q_cols, q_cols), q_cols)]
        return pltpu.make_async_remote_copy(view, view, a_send, a_recv.at[odd(u)], device_id={"sp": partner}, device_id_type=MESH)

    def lend_copies():
        rows_there = pl.ds(tokens, rows)
        return tuple(
            pltpu.make_async_remote_copy(
                src.at[u_rows(lent), :], qbuf.at[core, rows_there, :], lend_send.at[0, d], lend_recv.at[0, d], device_id={"sp": to}, device_id_type=MESH)
            for d, (src, to) in enumerate(((q_mine, across), (q_other, across_partner)))
        )

    def lent_copies():
        view = abuf.at[2, :, pl.ds(mult(core * q_cols, q_cols), q_cols)]
        return tuple(
            pltpu.make_async_remote_copy(view, view, lend_send.at[1, d], lend_recv.at[1, d], device_id={"sp": to}, device_id_type=MESH)
            for d, to in enumerate((across, across_partner))
        )

    def part(p):
        u = over(p, per_unit)
        i = p - u * per_unit
        return u, lax.shift_right_logical(i, 1), odd(i)

    def sum_view(p):
        u, b, r = part(p)
        return pbuf.at[odd(u), pl.ds(mult(r * rows, rows), rows), pl.ds(mult(b * bw, bw), bw)]

    def sum_copy(p):
        return pltpu.make_async_remote_copy(
            sum_view(p), rbuf.at[p & (SLOTS - 1)], rs_send.at[p & (SENDS - 1)], rs_recv.at[p & (SLOTS - 1)], device_id={"tp": z_next}, device_id_type=MESH)

    def y_view(owner, p):
        u, b, _ = part(p)
        return y_out.at[pl.ds(mult(u * rows, rows), rows), pl.ds(mult(owner * cols_half + b * bw, bw), bw)]

    def start_x(p):
        u, b, r = part(p)
        src = (pl.ds(mult(u * rows, rows), rows), pl.ds(mult(core * cols_half + b * bw, bw), bw))

        @pl.when(r == core)
        def _():
            pltpu.make_async_copy(x_own.at[src[0], src[1]], xbuf.at[odd(p)], x_sem.at[odd(p)]).start()

        @pl.when(r != core)
        def _():
            pltpu.make_async_copy(x_par.at[src[0], src[1]], xbuf.at[odd(p)], x_sem.at[odd(p)]).start()

    def near_local(p):
        return pltpu.make_async_copy(ybuf.at[p & (SENDS - 1)], y_view(core, p), y_near.at[p & (SENDS - 1)])

    def near_remote(p):
        return pltpu.make_async_remote_copy(
            ybuf.at[p & (SENDS - 1)], y_view(core, p), y_near.at[p & (SENDS - 1)], ag_recv.at[core, lax.shift_right_logical(p, 1)], device_id={"sp": partner}, device_id_type=MESH)

    def far_remote(p):
        _, _, r = part(p)
        return pltpu.make_async_remote_copy(
            ybuf.at[p & (SENDS - 1)], y_view(core, p), y_far.at[p & (SENDS - 1)], ag_recv.at[core, lax.shift_right_logical(p, 1)],
            device_id={"tp": z_prev, "sp": 2 * row_y + r}, device_id_type=MESH)

    def wait_result_out(p):
        near_local(p).wait()
        far_remote(p).wait_send()

    def back_copy(owner, q):
        view = y_view(owner, 2 * q)
        z_to = jnp.clip(z - 1 + 2 * owner, 0, end)
        return pltpu.make_async_remote_copy(view, view, ag_send.at[owner, q], ag_recv.at[owner, q], device_id={"tp": z_to}, device_id_type=MESH)

    def sum_op(p):
        view = sum_view(p)

        @pl.when(hop > 0)
        def _():
            sum_copy(p).wait_recv()
            u, b, r = part(p)
            at = (odd(u), pl.ds(mult(r * rows, rows), rows), pl.ds(mult(b * bw, bw), bw))
            pbuf[at] = pbuf[at] + rbuf[p & (SLOTS - 1)]

            @pl.when(p + SLOTS < pieces)
            def _():
                pl.semaphore_signal(credit, inc=1, device_id={"tp": z_prev}, device_id_type=MESH)

        @pl.when(hop < end)
        def _():
            @pl.when(p >= SENDS)
            def _():
                sum_copy(p - SENDS).wait_send()

            @pl.when(p >= SLOTS)
            def _():
                pl.semaphore_wait(credit, 1)

            sum_copy(p).start()

        @pl.when(hop == end)
        def _():
            @pl.when(p >= SENDS)
            def _():
                wait_result_out(p - SENDS)

            slot = p & (SENDS - 1)
            pltpu.make_async_copy(x_own.at[pl.ds(0, rows), pl.ds(0, bw)], xbuf.at[odd(p)], x_sem.at[odd(p)]).wait()
            ybuf[slot] = (xbuf[odd(p)].astype(F32) + view[...]).astype(BF16)

            @pl.when(p + 2 < pieces)
            def _():
                start_x(p + 2)

            far_remote(p).start()
            r = odd(p)

            @pl.when(r == core)
            def _():
                near_local(p).start()

            @pl.when(r != core)
            def _():
                near_remote(p).start()

    def back_op(owner, q, distance):
        back_copy(owner, q).wait_recv()

        @pl.when((distance > 0) & (distance < end))
        def _():
            back_copy(owner, q).start()

    def ticks(t, count):
        def body(i, carry):
            tick(t + i)
            return carry

        lax.fori_loop(0, count, body, 0)

    many, span_of = RATE

    def piece_at(v, span, per):
        v_ok = jnp.maximum(v, 0)
        u = over(v_ok, span)
        w = v_ok - u * span
        i = over(many * w + span_of - 1, span_of)
        return u * per + i, (v >= 0) & (span_of * i - many * w < many) & (i < per) & (u < units)

    first_back = 7 + end * HOP

    def tick(t):
        p, here = piece_at(t - 3 - hop * HOP, unit_ticks, per_unit)

        @pl.when(here)
        def _():
            sum_op(p)

        owner = odd(t)
        distance = jnp.where(owner == 0, end - z, z)
        q, back = piece_at(lax.shift_right_arithmetic(t - first_back - distance * BACK_HOP, 1), unit_ticks // 2, nbw)

        @pl.when(back & ((distance > 0) | (core != owner)))
        def _():
            back_op(owner, q, distance)

    last_tick = below(units) * unit_ticks + 2 * (span_of * nbw // many + 1) + first_back + end * BACK_HOP + 2

    def attend(first, token, slot, r, s):
        q_rows = qbuf[r, pl.ds(mult(first, att), att), :]
        q_stack = jnp.concatenate([q_rows[:, i * HEAD_DIM:(i + 1) * HEAD_DIM] for i in range(heads)], axis=0)
        m_buf[...] = jnp.full_like(m_buf, -jnp.inf)
        l_buf[...] = jnp.zeros_like(l_buf)
        acc_buf[...] = jnp.zeros_like(acc_buf)

        def stage(held, held_start, fresh, fresh_start, masked=False):
            if fresh is not None:
                start = mult(fresh_start, keys_step)
                part = lax.dot_general(kbuf[pl.ds(start, keys_step), :], q_stack, (((1,), (1,)), ((), ())), preferred_element_type=F32)
                if masked:
                    key_id = start + lax.broadcasted_iota(jnp.int32, part.shape, 0)
                    token_id = token + (lax.broadcasted_iota(jnp.int32, part.shape, 1) & (att - 1))
                    part = jnp.where(key_id <= token_id, part, -jnp.inf)
                fresh[...] = part
                top = jnp.max(part.reshape(keys_step // 8, 8, part.shape[1]), axis=0)
            if held is not None:
                m_old = m_buf[...]
                m_new = jnp.maximum(m_old, jnp.max(top_buf[...], axis=0, keepdims=True))
                m_buf[...] = m_new
                fade = jnp.exp2((m_old - m_new) * EXP2_SCALE)
                w = jnp.exp2((held[...] - m_new[0:1]) * EXP2_SCALE)
                l_buf[...] = l_buf[...] * fade + jnp.sum(w.reshape(keys_step // 8, 8, w.shape[1]), axis=0)
                acc_buf[...] = acc_buf[...] * fade[0:1] + jnp.dot(
                    vtbuf[:, pl.ds(mult(held_start, keys_step), keys_step)], w.astype(BF16), preferred_element_type=F32)
            if fresh is not None:
                top_buf[...] = top

        clear = token // keys_step
        edge = clear * keys_step
        stage(None, None, s0_buf, edge, True)

        def pair(i, carry):
            stage(s0_buf, jnp.where(i == 0, edge, (2 * i - 1) * keys_step), s1_buf, 2 * i * keys_step)
            stage(s1_buf, 2 * i * keys_step, s0_buf, (2 * i + 1) * keys_step)
            return carry

        pairs = clear // 2
        lax.fori_loop(0, pairs, pair, 0)
        held = jnp.where(pairs == 0, edge, (2 * pairs - 1) * keys_step)

        @pl.when(clear % 2 == 1)
        def _():
            stage(s0_buf, held, s1_buf, (clear - 1) * keys_step)
            stage(s1_buf, (clear - 1) * keys_step, None, None)

        @pl.when(clear % 2 == 0)
        def _():
            stage(s0_buf, held, None, None)

        out = (acc_buf[...] / jnp.sum(l_buf[...], axis=0, keepdims=True)).astype(BF16)
        for i in range(heads):
            abuf[slot, pl.ds(mult(r * rows + s * att, att), att), pl.ds(mult(core * q_cols + i * HEAD_DIM, HEAD_DIM), HEAD_DIM)] = out[:, i * att:(i + 1) * att].T

    start_gate_up(0)
    par_x_copy().start()
    own_u_copy(0).start()
    start_gate_up(1)
    for copy in own_copies():
        copy.start()
    own_cache().start()

    @pl.when(hop == end)
    def _():
        start_x(0)
        start_x(1)

    barrier = pltpu.get_barrier_semaphore()
    for other in (partner, across, across_partner):
        pl.semaphore_signal(barrier, inc=1, device_id={"sp": other}, device_id_type=MESH)

    @pl.when(z > 0)
    def _():
        pl.semaphore_signal(barrier, inc=1, device_id={"tp": z - 1}, device_id_type=MESH)
        pl.semaphore_signal(barrier, inc=1, device_id={"tp": z - 1, "sp": partner}, device_id_type=MESH)

    @pl.when(z < end)
    def _():
        pl.semaphore_signal(barrier, inc=1, device_id={"tp": z + 1}, device_id_type=MESH)
        pl.semaphore_signal(barrier, inc=1, device_id={"tp": z + 1, "sp": partner}, device_id_type=MESH)

    par_x_copy().wait()
    norm_par_rows()
    pl.semaphore_wait(barrier, 3 + 2 * (z > 0).astype(jnp.int32) + 2 * (z < end).astype(jnp.int32))

    for d in (1, 2, 0):
        for copy in key_copies(d):
            copy.start()
    q_copy().start()

    @pl.when(row_y == 1)
    def _():
        for copy in lend_copies():
            copy.start()

    def send_u(u, carry):
        far_u_copy(u).start()
        return carry

    lax.fori_loop(1, units, send_u, 0)

    def unit(u, carry):
        t0 = u * unit_ticks
        gate_up_tick = t0 - 2 * nbg - 2 * subs
        own_u_copy(u).wait()

        @pl.when(u > 0)
        def _():
            par_u_copy(u).wait()

        for n in range(DOWN_SLOTS):
            down_copy(n).start()
        out_copy(0).start()
        out_copy(1).start()

        def gate_up(n, carry):
            slot = odd(n)
            copy_g, copy_u = gate_up_copies(n)
            copy_g.wait()
            copy_u.wait()
            both = jnp.dot(ubuf[...], wgu_buf[slot], preferred_element_type=F32)
            hbuf[odd(u), :, pl.ds(mult(core * ff_half + n * bg, bg), bg)] = silu_mul(both[:, :bg], both[:, bg:])

            @pl.when(n + 2 < nbg)
            def _():
                start_gate_up(n + 2)

            ticks(gate_up_tick + 2 * n, 2)
            h_copy(u, n).start()
            return carry

        lax.fori_loop(0, nbg, gate_up, 0)

        @pl.when(u == 0)
        def _():
            for copy in own_copies():
                copy.wait()
            for d in range(3):
                for copy in key_copies(d):
                    copy.wait()
            q_copy().wait()
            for d in range(3):
                cache_copy(d).start()

        borrows = (row_y == 0) & (u == lent - 1)
        lends = (row_y == 1) & (u == lent)
        a_slot = jnp.where(lends, 2, odd(u))

        @pl.when(borrows)
        def _():
            for copy in lend_copies():
                copy.wait_recv()

        def sub(i, carry):
            mine = i < 2 * subs
            j = jnp.where(mine, i, i - 2 * subs)
            r = over(j, subs)
            part = j - r * subs
            first = jnp.where(mine, u * rows, tokens) + part * att
            token = jnp.where(mine, (2 * row_y + r) * tokens + u * rows, (2 + r) * tokens + lent * rows) + part * att
            attend(first, token, jnp.where(mine, odd(u), 2), r, part)
            ticks(t0 - 2 * subs + i, mine.astype(jnp.int32))
            return carry

        lax.fori_loop(0, jnp.where(lends, 0, jnp.where(borrows, 4 * subs, 2 * subs)), sub, 0)

        @pl.when(lends)
        def _():
            ticks(t0 - 2 * subs, 2 * subs)

        @pl.when(jnp.logical_not(lends))
        def _():
            a_copy(u).start()

        @pl.when(borrows)
        def _():
            for copy in lent_copies():
                copy.start()

        @pl.when(u + 1 < units)
        def _():
            own_u_copy(u + 1).start()
            far_u_copy(u + 1).wait()
            par_u_copy(u + 1).start()
            start_gate_up(0)
            start_gate_up(1)

        def wait_h(j, carry):
            h_copy(u, j).wait()
            return carry

        def down(b, carry):
            cols = pl.ds(mult(b * wb, wb), wb)
            own_rows = pl.ds(mult(core * ff_half, ff_half), ff_half)
            par_rows = pl.ds(mult((twin) * ff_half, ff_half), ff_half)
            down_copy(2 * b).wait()
            pbuf[odd(u), :, cols] = jnp.dot(hbuf[odd(u), :, own_rows], wd_buf[0], preferred_element_type=F32)

            @pl.when(b + 1 < nbw // 2)
            def _():
                down_copy(2 * b + 2).start()

            ticks(t0 + 4 * b, 2)

            @pl.when(b == 0)
            def _():
                lax.fori_loop(0, nbg, wait_h, 0)

                @pl.when(lends)
                def _():
                    for copy in lent_copies():
                        copy.wait_recv()

                @pl.when(jnp.logical_not(lends))
                def _():
                    a_copy(u).wait()

            down_copy(2 * b + 1).wait()
            out_copy(b).wait()
            pbuf[odd(u), :, cols] = (
                pbuf[odd(u), :, cols]
                + jnp.dot(hbuf[odd(u), :, par_rows], wd_buf[1], preferred_element_type=F32)
                + jnp.dot(abuf[a_slot], wo_buf[odd(b)], preferred_element_type=F32)
            )

            @pl.when(b + 1 < nbw // 2)
            def _():
                down_copy(2 * b + 3).start()

            @pl.when(b + 2 < nbw // 2)
            def _():
                out_copy(b + 2).start()

            ticks(t0 + 4 * b + 2, 2)
            return carry

        lax.fori_loop(0, nbw // 2, down, 0)
        return carry

    lax.fori_loop(0, units, unit, 0)

    def drain(t, carry):
        tick(t)
        return carry

    lax.fori_loop(below(units) * unit_ticks + 2 * nbw, last_tick + 1, drain, 0)

    def sums_out(i, carry):
        p = pieces - SENDS + i

        @pl.when(hop < end)
        def _():
            sum_copy(p).wait_send()

        @pl.when(hop == end)
        def _():
            wait_result_out(p)

        return carry

    lax.fori_loop(0, SENDS, sums_out, 0)

    for owner in (0, 1):
        distance = end - z if owner == 0 else z

        @pl.when((distance > 0) & (distance < end))
        def _():
            def backs_out(q, carry):
                back_copy(owner, q).wait_send()
                return carry

            lax.fori_loop(0, pieces // 2, backs_out, 0)

    own_cache().wait()
    for d in range(3):
        cache_copy(d).wait()

    @pl.when(row_y == 1)
    def _():
        for copy in lend_copies():
            copy.wait_send()

    @pl.when(row_y == 0)
    def _():
        for copy in lent_copies():
            copy.wait_send()


def layer(u_own, x_own, x_par, gain, q_mine, q_other, kv, vt, w_gate, w_up, w_down, w_o):
    tokens, model = u_own.shape
    ff = w_gate.shape[1]
    ff_half, cols_half = ff // 2, model // 2
    rows = tokens // 4
    att = min(128, rows)
    bg, bw = block_of(ff_half, 256), block_of(cols_half, 512) // 2
    wb = 2 * bw
    nbg, nbw = ff_half // bg, cols_half // bw
    q_cols = q_mine.shape[1]
    kv_tokens = 4 * tokens
    keys_step = min(512, kv_tokens // 4)
    units = tokens // rows
    pieces = 2 * nbw * units
    stack = att * (q_cols // HEAD_DIM)
    any_spec = pl.BlockSpec(memory_space=pl.ANY)
    dma = pltpu.SemaphoreType.DMA
    two, sends, quad, peer = dma((2,)), dma((SENDS,)), dma((2, 2)), dma((3, 3))
    macs = tokens * model * (3 * ff + w_o.shape[0])
    y_out, cache, _ = pl.pallas_call(
        functools.partial(layer_kernel, rows, att, keys_step),
        out_shape=[
            jax.ShapeDtypeStruct((tokens, model), BF16),
            jax.ShapeDtypeStruct((kv_tokens, 2 * HEAD_DIM), BF16),
            jax.ShapeDtypeStruct((tokens, model), BF16),
        ],
        in_specs=[any_spec] * 3 + [pl.BlockSpec(memory_space=pltpu.VMEM)] + [any_spec] * 8,
        out_specs=[any_spec] * 3,
        scratch_shapes=[
            pltpu.VMEM((2, model, 2 * bg), BF16),
            pltpu.VMEM((DOWN_SLOTS, ff_half, wb), BF16),
            pltpu.VMEM((2, w_o.shape[0], wb), BF16),
            pltpu.VMEM((2 * rows, model), BF16),
            pltpu.VMEM((2, 2 * rows, ff), BF16),
            pltpu.VMEM((3, 2 * rows, w_o.shape[0]), BF16),
            pltpu.VMEM((2, tokens + rows, q_cols), BF16),
            pltpu.VMEM((kv_tokens, HEAD_DIM), BF16),
            pltpu.VMEM((HEAD_DIM, kv_tokens), BF16),
            pltpu.VMEM((2, 2 * rows, cols_half), F32),
            pltpu.VMEM((SLOTS, rows, bw), F32),
            pltpu.VMEM((2, rows, bw), BF16),
            pltpu.VMEM((SENDS, rows, bw), BF16),
            pltpu.VMEM((8, stack), F32),
            pltpu.VMEM((8, stack), F32),
            pltpu.VMEM((HEAD_DIM, stack), F32),
            pltpu.VMEM((keys_step, stack), F32),
            pltpu.VMEM((keys_step, stack), F32),
            pltpu.VMEM((8, stack), F32),
            quad, dma((DOWN_SLOTS,)), two, two, dma((4,)), dma((units,)), dma((units,)), dma, dma, peer, peer,
            dma((nbg,)), dma((2, nbg)), dma, two, quad, quad,
            sends, dma((SLOTS,)), sends, sends, sends,
            dma((2, pieces // 2)), dma((2, pieces // 2)),
            pltpu.SemaphoreType.REGULAR,
        ],
        compiler_params=pltpu.CompilerParams(
            collective_id=0, has_side_effects=True, vmem_limit_bytes=VMEM_BYTES),
        cost_estimate=pl.CostEstimate(flops=macs, bytes_accessed=6 * ff_half * model * units, transcendentals=0),
        name="layer",
    )(u_own, x_own, x_par, gain, q_mine, q_other, kv, vt, w_gate, w_up, w_down, w_o)
    return y_out, cache


def finish_kernel(y_in, cache_in, y_out, k_out, v_out, y_buf, cache_buf, in_sem, out_sem):
    parts = in_sem.shape[0] // 2
    y_rows, cache_rows = y_in.shape[0] // parts, cache_in.shape[0] // parts
    keys, values = pl.ds(0, HEAD_DIM), pl.ds(HEAD_DIM, HEAD_DIM)

    def copies(i):
        rows = pl.ds(i * y_rows, y_rows)
        lines = pl.ds(i * cache_rows, cache_rows)
        y_sem, c_sem = in_sem.at[i], in_sem.at[parts + i]
        return (
            (pltpu.make_async_copy(y_in.at[rows], y_buf.at[rows], y_sem), pltpu.make_async_copy(cache_in.at[lines], cache_buf.at[lines], c_sem)),
            (
                pltpu.make_async_copy(y_buf.at[rows], y_out.at[rows], out_sem.at[i]),
                pltpu.make_async_copy(cache_buf.at[lines, keys], k_out.at[lines], out_sem.at[parts + i]),
                pltpu.make_async_copy(cache_buf.at[lines, values], v_out.at[lines], out_sem.at[parts + parts + i]),
            ),
        )

    every = [copies(i) for i in range(parts)]
    for ins, _ in every:
        for copy in ins:
            copy.start()
    for ins, outs in every:
        for copy in ins:
            copy.wait()
        for copy in outs:
            copy.start()
    for _, outs in every:
        for copy in outs:
            copy.wait()


def finish(y, cache):
    parts = 8
    head = jax.ShapeDtypeStruct((cache.shape[0], HEAD_DIM), BF16)
    any_spec = pl.BlockSpec(memory_space=pl.ANY)
    return pl.pallas_call(
        finish_kernel,
        out_shape=[jax.ShapeDtypeStruct(y.shape, BF16), head, head],
        in_specs=[any_spec] * 2,
        out_specs=[any_spec] * 3,
        scratch_shapes=[
            pltpu.VMEM(y.shape, BF16),
            pltpu.VMEM(cache.shape, BF16),
            pltpu.SemaphoreType.DMA((2 * parts,)),
            pltpu.SemaphoreType.DMA((3 * parts,)),
        ],
        compiler_params=pltpu.CompilerParams(vmem_limit_bytes=VMEM_BYTES),
        name="finish",
    )(y, cache)


def solution(mesh):
    row_spec = P(("rep", "sp"), None)
    cache_spec = P("rep", ("tp", "sp"), None)
    other_core = [(0, 1), (1, 0), (2, 3), (3, 2)]

    def layer_block(x_in, positions, norm_gain, w_q, w_k, w_v, w_o, w_gate, w_up, w_down):
        core = (lax.axis_index("sp") % 2).astype(jnp.int32).reshape(1)
        x_par = lax.ppermute(x_in, "sp", other_core)
        cos_tab, sin_tab = rope_tables(positions)
        gain = norm_gain.reshape(1, -1)
        normed, kv, vt, q_other, q_mine = project(core, x_in, gain, cos_tab, sin_tab, w_k, w_v, w_q)
        y_out, cache = layer(normed, x_in, x_par, gain, q_mine, q_other, kv, vt, w_gate, w_up, w_down, w_o)
        y_out, k_cache, v_cache = finish(y_out, cache)
        return y_out, k_cache[:, None], v_cache[:, None]

    return jax.shard_map(
        layer_block,
        mesh=mesh,
        in_specs=(row_spec, P(("rep", "sp")), P(None), P(None, "tp"), P(None, "tp"), P(None, "tp"), P("tp", None), P(None, "tp"), P(None, "tp"), P("tp", None)),
        out_specs=(row_spec, cache_spec, cache_spec),
        check_vma=False,
    )
```
